32 devices in a mesh: dp: 4 (over y, z), ep: 8 (over x, core).
Axes of the slice: x: 4, y: 2, z: 2, core: 2. Of those that a mesh axis runs over, the one named last changes fastest.
The devices are a block of a 4x4x8 slice.
Arguments:
- x_in: bfloat16 [8192, 1024], P(('dp', 'ep')), parts along dimension 0
- k_cache: bfloat16 [8192, 32, 8, 64], P(('dp', 'ep')), parts along dimension 0
- v_cache: bfloat16 [8192, 32, 8, 64], P(('dp', 'ep')), parts along dimension 0
- cache_len: int32 [8192], P(('dp', 'ep')), parts along dimension 0
- topk_idx: int32 [8192, 8], P(('dp', 'ep')), parts along dimension 0
- ln_attn: bfloat16 [1024], replicated
- w_q: bfloat16 [1024, 1024], replicated
- w_k: bfloat16 [1024, 512], replicated
- w_v: bfloat16 [1024, 512], replicated
- q_norm: bfloat16 [64], replicated
- k_norm: bfloat16 [64], replicated
- w_o: bfloat16 [1024, 1024], replicated
- ln_moe: bfloat16 [1024], replicated
- w_router: bfloat16 [1024, 32], replicated
- w_gate: bfloat16 [32, 1024, 512], P('ep')
- w_up: bfloat16 [32, 1024, 512], P('ep')
- w_down: bfloat16 [32, 512, 1024], P('ep')
Outputs:
- output 1: bfloat16 [8192, 1024], P(('dp', 'ep')), parts along dimension 0
- output 2: bfloat16 [8192, 32, 8, 64], P(('dp', 'ep')), parts along dimension 0
- output 3: bfloat16 [8192, 32, 8, 64], P(('dp', 'ep')), parts along dimension 0
There are 4 independent parts. The reference program is written for one: setup_inputs(seed, part) draws one part's arguments, and reference() takes and returns one part's arrays. A program takes and returns all parts, laid end to end along the dimension named above; an argument that names none is the same for every part.
All inputs are finite; a program needn't handle non-finite values.
Results may differ from the reference program's by a relative error of at most 0.0140908.
Values are sent between devices in bfloat16 or wider.
A program may use at most 768 MiB of HBM per device.

```python
import jax
import jax.numpy as jnp
import numpy as np
from jax import lax

HIDDEN = 1024
Q_HEADS = 16
KV_HEADS = 8
HEAD_DIM = 64
EXPERTS = 32
TOP_K = 8
EXPERT_FF = 512
B_DEV = 256
CACHE_LEN = 32
EP_SIZE = 8
BATCH = B_DEV * EP_SIZE
E_LOCAL = EXPERTS // EP_SIZE
ROPE_BASE = 1000000.0
NORM_EPS = 1e-6


def draw_layout(len_key, route_key, local_key):
    pair_count = B_DEV * TOP_K
    cap_rows = min(B_DEV, 2 * pair_count // EP_SIZE)
    n_hot = EP_SIZE // TOP_K
    n_cold = EP_SIZE - n_hot
    rest_rows = pair_count - n_hot * cap_rows
    base_rows = rest_rows // n_cold
    extra_rows = rest_rows - base_rows * n_cold
    row_counts = [cap_rows] * n_hot + [base_rows + 1] * extra_rows + [base_rows] * (n_cold - extra_rows)
    rank_table = np.repeat(np.arange(EP_SIZE), row_counts).reshape(TOP_K, B_DEV).T
    dev_keys = jax.random.split(route_key, EP_SIZE + 1)
    dev_perm = jax.random.permutation(dev_keys[0], EP_SIZE)
    row_perms = jax.vmap(lambda key_one: jax.random.permutation(key_one, B_DEV))(dev_keys[1:])
    dev_table = dev_perm[jnp.asarray(rank_table)]
    dev_all = dev_table[row_perms]
    local_ids = jax.random.randint(local_key, (EP_SIZE, B_DEV, TOP_K), 0, E_LOCAL)
    topk_idx = (dev_all * E_LOCAL + local_ids).reshape(BATCH, TOP_K).astype(jnp.int32)
    len_keys = jax.random.split(len_key, 3)
    shard_top = jax.random.randint(len_keys[0], (EP_SIZE, 1), CACHE_LEN // 4, CACHE_LEN)
    len_draw = jax.random.randint(len_keys[1], (EP_SIZE, B_DEV), 1, shard_top).reshape(BATCH)
    longest = jax.random.randint(len_keys[2], (), 0, BATCH)
    cache_len = jnp.where(jnp.arange(BATCH) == longest, CACHE_LEN - 1, len_draw).astype(jnp.int32)
    return cache_len, topk_idx


def setup_inputs(seed: int = 0, part: int = 0) -> dict:
    base_key = jax.random.key(seed)
    part_keys = jax.random.split(jax.random.fold_in(base_key, part), 6)
    shared_keys = jax.random.split(base_key, 14)
    q_width = Q_HEADS * HEAD_DIM
    kv_width = KV_HEADS * HEAD_DIM

    def normal_of(rand_key, arr_shape, scale_mul):
        return jax.random.normal(rand_key, arr_shape, jnp.float32) * scale_mul

    cache_len, topk_idx = draw_layout(part_keys[3], part_keys[4], part_keys[5])
    cache_shape = (BATCH, CACHE_LEN, KV_HEADS, HEAD_DIM)
    return {
        'x_in': normal_of(part_keys[0], (BATCH, HIDDEN), 1.0).astype(jnp.bfloat16),
        'k_cache': normal_of(part_keys[1], cache_shape, 1.5).astype(jnp.bfloat16),
        'v_cache': normal_of(part_keys[2], cache_shape, 1.0).astype(jnp.bfloat16),
        'cache_len': cache_len,
        'topk_idx': topk_idx,
        'ln_attn': (1.0 + normal_of(shared_keys[0], (HIDDEN,), 0.3)).astype(jnp.bfloat16),
        'w_q': normal_of(shared_keys[1], (HIDDEN, q_width), HIDDEN ** -0.5).astype(jnp.bfloat16),
        'w_k': normal_of(shared_keys[2], (HIDDEN, kv_width), HIDDEN ** -0.5).astype(jnp.bfloat16),
        'w_v': normal_of(shared_keys[3], (HIDDEN, kv_width), HIDDEN ** -0.5).astype(jnp.bfloat16),
        'q_norm': (2.0 + normal_of(shared_keys[4], (HEAD_DIM,), 0.4)).astype(jnp.bfloat16),
        'k_norm': (2.0 + normal_of(shared_keys[5], (HEAD_DIM,), 0.4)).astype(jnp.bfloat16),
        'w_o': normal_of(shared_keys[6], (q_width, HIDDEN), q_width ** -0.5).astype(jnp.bfloat16),
        'ln_moe': (1.0 + normal_of(shared_keys[7], (HIDDEN,), 0.3)).astype(jnp.bfloat16),
        'w_router': normal_of(shared_keys[8], (HIDDEN, EXPERTS), 1.5 * HIDDEN ** -0.5).astype(jnp.bfloat16),
        'w_gate': normal_of(shared_keys[9], (EXPERTS, HIDDEN, EXPERT_FF), HIDDEN ** -0.5).astype(jnp.bfloat16),
        'w_up': normal_of(shared_keys[10], (EXPERTS, HIDDEN, EXPERT_FF), HIDDEN ** -0.5).astype(jnp.bfloat16),
        'w_down': normal_of(shared_keys[11], (EXPERTS, EXPERT_FF, HIDDEN), 3.0 * EXPERT_FF ** -0.5).astype(jnp.bfloat16),
    }


def norm_scale(values, gain_vec):
    return values * lax.rsqrt(jnp.mean(values * values, axis=-1, keepdims=True) + NORM_EPS) * gain_vec.astype(jnp.float32)


def rotate_halves(values, positions):
    half_dim = values.shape[-1] // 2
    freq_vec = ROPE_BASE ** (-jnp.arange(half_dim, dtype=jnp.float32) * 2.0 / values.shape[-1])
    angles = positions.astype(jnp.float32)[:, None, None] * freq_vec
    cosine = jnp.cos(angles)
    sine_val = jnp.sin(angles)
    lo_half = values[..., :half_dim]
    hi_half = values[..., half_dim:]
    return jnp.concatenate([lo_half * cosine - hi_half * sine_val, hi_half * cosine + lo_half * sine_val], axis=-1)


def reference(x_in, k_cache, v_cache, cache_len, topk_idx, ln_attn, w_q, w_k, w_v, q_norm, k_norm, w_o, ln_moe, w_router, w_gate, w_up, w_down):
    resid_in = x_in.astype(jnp.float32)
    normed = norm_scale(resid_in, ln_attn).astype(jnp.bfloat16)
    q_proj = jnp.dot(normed, w_q, preferred_element_type=jnp.float32).reshape(BATCH, Q_HEADS, HEAD_DIM)
    k_proj = jnp.dot(normed, w_k, preferred_element_type=jnp.float32).reshape(BATCH, KV_HEADS, HEAD_DIM)
    v_new = jnp.dot(normed, w_v, preferred_element_type=jnp.float32).astype(jnp.bfloat16).reshape(BATCH, KV_HEADS, HEAD_DIM)
    q_rot = rotate_halves(norm_scale(q_proj, q_norm), cache_len).astype(jnp.bfloat16)
    k_new = rotate_halves(norm_scale(k_proj, k_norm), cache_len).astype(jnp.bfloat16)
    slot_ids = jnp.arange(CACHE_LEN)
    is_new = slot_ids[None, :, None, None] == cache_len[:, None, None, None]
    k_full = jnp.where(is_new, k_new[:, None], k_cache)
    v_full = jnp.where(is_new, v_new[:, None], v_cache)

    def one_token(args_tok):
        q_tok, k_tok, v_tok, len_tok = args_tok
        q_grp = q_tok.reshape(KV_HEADS, Q_HEADS // KV_HEADS, HEAD_DIM).astype(jnp.float32)
        scores = jnp.einsum('grd,sgd->grs', q_grp, k_tok.astype(jnp.float32)) * HEAD_DIM ** -0.5
        scores = jnp.where(slot_ids <= len_tok, scores, -1e30)
        attn_prob = jax.nn.softmax(scores, axis=-1).astype(jnp.bfloat16)
        mixed = jnp.einsum('grs,sgd->grd', attn_prob.astype(jnp.float32), v_tok.astype(jnp.float32))
        return mixed.astype(jnp.bfloat16).reshape(Q_HEADS * HEAD_DIM)

    attn_out = lax.map(one_token, (q_rot, k_full, v_full, cache_len))
    x_mid = (resid_in + jnp.dot(attn_out, w_o, preferred_element_type=jnp.float32)).astype(jnp.bfloat16)
    resid_mid = x_mid.astype(jnp.float32)
    h_moe = norm_scale(resid_mid, ln_moe).astype(jnp.bfloat16)
    logits = jnp.dot(h_moe, w_router, preferred_element_type=jnp.float32)
    route_prob = jax.nn.softmax(logits, axis=-1)
    picked = jnp.take_along_axis(route_prob, topk_idx, axis=1)
    gate_wts = picked / jnp.sum(picked, axis=1, keepdims=True)
    tok_rows = jnp.repeat(h_moe, TOP_K, axis=0)

    def one_pair(args_pair):
        row_vec, expert = args_pair
        row_mat = row_vec[None, :]
        gate_act = jnp.dot(row_mat, w_gate[expert], preferred_element_type=jnp.float32)
        up_act = jnp.dot(row_mat, w_up[expert], preferred_element_type=jnp.float32)
        hidden_act = (jax.nn.silu(gate_act) * up_act).astype(jnp.bfloat16)
        return jnp.dot(hidden_act, w_down[expert], preferred_element_type=jnp.float32).astype(jnp.bfloat16)[0]

    expert_out = lax.map(one_pair, (tok_rows, topk_idx.reshape(BATCH * TOP_K)))
    moe_out = jnp.sum(expert_out.reshape(BATCH, TOP_K, HIDDEN).astype(jnp.float32) * gate_wts[:, :, None], axis=1)
    x_out = (resid_mid + moe_out).astype(jnp.bfloat16)
    return x_out, k_full, v_full
```

```python
import functools

import jax
import jax.numpy as jnp
import numpy as np
from jax import lax
from jax.experimental import pallas as pl
from jax.experimental.pallas import tpu as pltpu
from jax.sharding import PartitionSpec as P

ROPE_BASE = 1000000.0
NORM_EPS = 1e-6
F32 = jnp.float32
BF16 = jnp.bfloat16
MESH = pl.DeviceIdType.MESH


def attn_kernel(freq_ref, x_ref, len_ref, topk_ref, lna_ref, qn_ref, kn_ref, wq_ref, wk_ref, wv_ref, wo_hbm, lnm_ref, wr_ref, kc_ref, vc_ref,
                x1_ref, h2_ref, ri_ref, kco_ref, vco_ref,
                h_scr, cos_scr, sin_scr, qg_scr, kg_scr, len_scr, q_scr, kn_scr, vn_scr, s_scr, o_scr, wo_scr, wo_sem):
    step = pl.program_id(0)
    last = pl.num_programs(0) - 1
    n_tok = x_ref.shape[0]
    n_slots, _, head_dim, _ = kc_ref.shape
    half = head_dim // 2
    n_lt = n_tok // 128
    wo_copy = pltpu.make_async_copy(wo_hbm, wo_scr, wo_sem)

    @pl.when(step == 0)
    def _():
        wo_copy.start()
        xf = x_ref[...].astype(F32)
        ms = jnp.mean(xf * xf, axis=1, keepdims=True)
        h_scr[...] = (xf * lax.rsqrt(ms + NORM_EPS) * lna_ref[...].astype(F32)).astype(BF16)
        lens = len_ref[...].astype(F32)
        freq = jnp.concatenate([freq_ref[...]] * n_lt, axis=1)
        angles = freq * lens
        cos_scr[...] = jnp.cos(angles)
        sin_scr[...] = jnp.sin(angles)
        for src, dst in ((qn_ref, qg_scr), (kn_ref, kg_scr)):
            row = src[...].astype(F32)
            wide = jnp.broadcast_to(jnp.concatenate([row, row], axis=1), (128, 128))
            dst[...] = wide.T[:head_dim]
        len_scr[...] = jnp.broadcast_to(lens, (head_dim, n_tok)).astype(BF16)

    def head_rope(block, gain_scr):
        ms = jnp.mean(block * block, axis=0, keepdims=True)
        gain = jnp.concatenate([gain_scr[...]] * n_lt, axis=1)
        block = block * lax.rsqrt(ms + NORM_EPS) * gain
        lo, hi = block[:half], block[half:]
        cosv, sinv = cos_scr[...], sin_scr[...]
        return jnp.concatenate([lo * cosv - hi * sinv, hi * cosv + lo * sinv], axis=0).astype(BF16)

    q_t = jnp.dot(h_scr[...], wq_ref[...], preferred_element_type=F32).T
    for j in range(2):
        q_scr[j] = head_rope(q_t[j * head_dim:(j + 1) * head_dim], qg_scr).astype(F32)

    @pl.when(step % 2 == 0)
    def _():
        k_t = jnp.dot(h_scr[...], wk_ref[...], preferred_element_type=F32).T
        v_t = jnp.dot(h_scr[...], wv_ref[...], preferred_element_type=F32).T
        for j in range(2):
            kn_scr[j] = head_rope(k_t[j * head_dim:(j + 1) * head_dim], kg_scr)
            vn_scr[j] = v_t[j * head_dim:(j + 1) * head_dim].astype(BF16)

    par = step % 2
    for lt in range(n_lt):
        lanes = pl.ds(lt * 128, 128)

        def score_block(i, carry):
            rows = [[], []]
            for si in range(8):
                s = i * 8 + si
                hit = len_scr[:, lanes] == s.astype(F32).astype(BF16)
                kb = jnp.where(hit, kn_scr[par, :, lanes], kc_ref[s, 0, :, lanes])
                kco_ref[s, 0, :, lanes] = kb
                kf = kb.astype(F32)
                for j in range(2):
                    rows[j].append(jnp.sum(kf * q_scr[j, :, lanes], axis=0, keepdims=True))
            for j in range(2):
                s_scr[j, pl.ds(pl.multiple_of(i * 8, 8), 8), lanes] = jnp.concatenate(rows[j], axis=0)
            return carry

        lax.fori_loop(0, n_slots // 8, score_block, 0)
        lens = len_ref[:, lanes]
        seen = lax.broadcasted_iota(jnp.int32, (n_slots, 128), 0) <= lens
        for j in range(2):
            sc = jnp.where(seen, s_scr[j, :, lanes] * (head_dim ** -0.5), -1e30)
            ex = jnp.exp(sc - jnp.max(sc, axis=0, keepdims=True))
            pr = ex / jnp.sum(ex, axis=0, keepdims=True)
            s_scr[j, :, lanes] = pr.astype(BF16).astype(F32)

        def value_block(i, accs):
            accs = list(accs)
            prob = [s_scr[j, pl.ds(pl.multiple_of(i * 8, 8), 8), lanes] for j in range(2)]
            for si in range(8):
                s = i * 8 + si
                hit = len_scr[:, lanes] == s.astype(F32).astype(BF16)
                vb = jnp.where(hit, vn_scr[par, :, lanes], vc_ref[s, 0, :, lanes])
                vco_ref[s, 0, :, lanes] = vb
                vf = vb.astype(F32)
                for j in range(2):
                    accs[j] = accs[j] + prob[j][si:si + 1] * vf
            return tuple(accs)

        zero = jnp.zeros((head_dim, 128), F32)
        accs = lax.fori_loop(0, n_slots // 8, value_block, (zero, zero))
        o_scr[pl.ds(lt * 128, 128), pl.ds(pl.multiple_of(step * 128, 128), 128)] = jnp.concatenate(accs, axis=0).T.astype(BF16)

    @pl.when(step == last)
    def _():
        wo_copy.wait()
        x1 = (x_ref[...].astype(F32) + jnp.dot(o_scr[...], wo_scr[...], preferred_element_type=F32)).astype(BF16)
        x1_ref[...] = x1
        xf = x1.astype(F32)
        ms = jnp.mean(xf * xf, axis=1, keepdims=True)
        h2 = (xf * lax.rsqrt(ms + NORM_EPS) * lnm_ref[...].astype(F32)).astype(BF16)
        h2_ref[...] = h2
        logits = lax.dot_general(wr_ref[...], h2, (((1,), (1,)), ((), ())), preferred_element_type=F32)
        top_k = topk_ref.shape[0]
        n_exp = wr_ref.shape[0]
        n_dev = ri_ref.shape[1]
        e_local = n_exp // n_dev
        exp_id = lax.broadcasted_iota(jnp.int32, (n_exp, n_tok), 0)
        picked = [jnp.sum(jnp.where(exp_id == topk_ref[pl.ds(k, 1), :], logits, 0.0), axis=0, keepdims=True) for k in range(top_k)]
        picked = jnp.concatenate(picked, axis=0)
        ex = jnp.exp(picked - jnp.max(picked, axis=0, keepdims=True))
        gate = ex / jnp.sum(ex, axis=0, keepdims=True)
        dev_id = lax.broadcasted_iota(jnp.int32, (n_dev, n_tok), 0)
        r_dev = jnp.zeros((n_dev, n_tok), F32)
        i_dev = jnp.zeros((n_dev, n_tok), F32)
        for k in range(top_k):
            idx = topk_ref[pl.ds(k, 1), :]
            dev = idx // e_local
            mine = dev_id == dev
            r_dev = r_dev + jnp.where(mine, gate[k:k + 1], 0.0)
            i_dev = i_dev + jnp.where(mine, (idx - dev * e_local).astype(F32), 0.0)
        ri_ref[0] = r_dev
        ri_ref[1] = i_dev


def attention(x_in, k_cache, v_cache, cache_len, topk_idx, ln_attn, w_q, w_k, w_v, q_norm, k_norm, w_o, ln_moe, w_router, ep_size):
    n_tok, hidden = x_in.shape
    _, n_slots, kv_heads, head_dim = k_cache.shape
    freq = np.float32(ROPE_BASE) ** (-np.arange(head_dim // 2, dtype=np.float32) * np.float32(2.0) / np.float32(head_dim))
    freq = jnp.asarray(np.ascontiguousarray(np.broadcast_to(freq[:, None], (head_dim // 2, 128))), F32)
    kt = k_cache.transpose(1, 2, 3, 0)
    vt = v_cache.transpose(1, 2, 3, 0)
    whole = lambda shape: pl.BlockSpec(shape, lambda p: (0,) * len(shape))
    cache_spec = pl.BlockSpec((n_slots, 1, head_dim, n_tok), lambda p: (0, p, 0, 0))
    pair_spec = pl.BlockSpec((hidden, 128), lambda p: (0, p // 2))
    out = pl.pallas_call(
        attn_kernel,
        grid=(kv_heads,),
        in_specs=[
            whole(freq.shape), whole((n_tok, hidden)), whole((1, n_tok)), whole((topk_idx.shape[1], n_tok)), whole((1, hidden)), whole((1, head_dim)), whole((1, head_dim)),
            pl.BlockSpec((hidden, 128), lambda p: (0, p)), pair_spec, pair_spec, pl.BlockSpec(memory_space=pl.ANY), whole((1, hidden)), whole((w_router.shape[1], hidden)),
            cache_spec, cache_spec,
        ],
        out_specs=[whole((n_tok, hidden)), whole((n_tok, hidden)), whole((2, ep_size, n_tok)), cache_spec, cache_spec],
        out_shape=[
            jax.ShapeDtypeStruct((n_tok, hidden), BF16), jax.ShapeDtypeStruct((n_tok, hidden), BF16), jax.ShapeDtypeStruct((2, ep_size, n_tok), F32),
            jax.ShapeDtypeStruct(kt.shape, BF16), jax.ShapeDtypeStruct(vt.shape, BF16),
        ],
        scratch_shapes=[
            pltpu.VMEM((n_tok, hidden), BF16), pltpu.VMEM((head_dim // 2, n_tok), F32), pltpu.VMEM((head_dim // 2, n_tok), F32),
            pltpu.VMEM((head_dim, 128), F32), pltpu.VMEM((head_dim, 128), F32), pltpu.VMEM((head_dim, n_tok), BF16),
            pltpu.VMEM((2, head_dim, n_tok), F32), pltpu.VMEM((2, head_dim, n_tok), BF16), pltpu.VMEM((2, head_dim, n_tok), BF16),
            pltpu.VMEM((2, n_slots, n_tok), F32), pltpu.VMEM((n_tok, w_q.shape[1]), BF16), pltpu.VMEM(w_o.shape, BF16), pltpu.SemaphoreType.DMA,
        ],
        name="attend",
    )(freq, x_in, cache_len.reshape(1, n_tok), topk_idx.T, ln_attn.reshape(1, hidden), q_norm.reshape(1, head_dim), k_norm.reshape(1, head_dim),
      w_q, w_k, w_v, w_o, ln_moe.reshape(1, hidden), w_router.T, kt, vt)
    x1, h2, ri, kto, vto = out
    return x1, h2, ri, kto.transpose(3, 0, 1, 2), vto.transpose(3, 0, 1, 2)


def moe_kernel(n_chip, h2_ref, ri_ref, x1_ref, wg_hbm, wu_hbm, wd_hbm, out_ref,
               wg, wu, wd, hbuf, gbuf, xm, gm, m_scr, ybuf, y_near, y_far, y_peer, y_own, s_out, s_in,
               w_sem, send_h, recv_h, send_p, recv_p, send_g, recv_g, send_n, recv_n, send_f, recv_f, send_y, recv_y, send_s, recv_s):
    ep = lax.axis_index("ep")
    core = lax.rem(ep, 2)
    chip = ep // 2
    right = lax.rem(chip + 1, n_chip)
    left = lax.rem(chip + n_chip - 1, n_chip)
    opp = lax.rem(chip + 2, n_chip)
    other = 1 - core
    n_tok, hidden = h2_ref.shape
    hb = n_tok // 2
    e_local = wg.shape[0] // hidden
    ff = wg.shape[1]

    def dev(ch, co):
        return {"ep": ch * 2 + co}

    def rcopy(src, dst, ssem, rsem, ch, co):
        return pltpu.make_async_remote_copy(src_ref=src, dst_ref=dst, send_sem=ssem, recv_sem=rsem, device_id=dev(ch, co), device_id_type=MESH)

    top = pl.ds(0, hb)
    bot = pl.ds(hb, hb)

    w_copies = [pltpu.make_async_copy(wg_hbm, wg, w_sem.at[0]), pltpu.make_async_copy(wu_hbm, wu, w_sem.at[1]), pltpu.make_async_copy(wd_hbm, wd, w_sem.at[2])]

    dispatch = {
        1: rcopy(h2_ref.at[top], hbuf.at[1, top], send_h.at[1], recv_h.at[1], right, core),
        2: rcopy(h2_ref.at[bot], hbuf.at[2, top], send_h.at[2], recv_h.at[2], left, core),
        5: rcopy(h2_ref.at[bot], hbuf.at[5, top], send_h.at[5], recv_h.at[5], right, core),
        6: rcopy(h2_ref.at[top], hbuf.at[6, top], send_h.at[6], recv_h.at[6], left, core),
        3: rcopy(hbuf.at[1, top], hbuf.at[3, top], send_h.at[3], recv_h.at[3], right, core),
        4: rcopy(hbuf.at[2, top], hbuf.at[4, top], send_h.at[4], recv_h.at[4], left, core),
    }
    to_peer = {u: rcopy(hbuf.at[u, top], hbuf.at[u, bot], send_p.at[u], recv_p.at[u], chip, other) for u in range(1, 7)}
    to_peer[7] = rcopy(h2_ref, hbuf.at[7], send_p.at[7], recv_p.at[7], chip, other)
    gate = []
    for u, hf, ch in ((1, 0, right), (2, 1, left), (3, 0, opp), (4, 1, opp), (5, 1, right), (6, 0, left)):
        for q, co in ((0, core), (1, other)):
            gate.append(rcopy(ri_ref.at[:, :, pl.ds(hf * hb, hb)], gbuf.at[u, :, :, pl.ds(q * hb, hb)], send_g.at[2 * u + q], recv_g.at[2 * u + q], ch, co))
    gate.append(rcopy(ri_ref, gbuf.at[7], send_g.at[14], recv_g.at[14], chip, other))

    near = {}
    far = {}
    for u, ch, slot in ((1, left, 0), (2, right, 1)):
        near[u] = [rcopy(ybuf.at[u, top], y_near.at[slot, core], send_n.at[slot, 0], recv_n.at[slot, core], ch, core),
                   rcopy(ybuf.at[u, bot], y_near.at[slot, core], send_n.at[slot, 1], recv_n.at[slot, core], ch, other)]
    for u, ch, slot in ((3, right, 1), (4, left, 0)):
        far[u] = [rcopy(ybuf.at[u, top], y_far.at[slot, core], send_f.at[slot, 0], recv_f.at[slot, core], ch, core),
                  rcopy(ybuf.at[u, bot], y_far.at[slot, core], send_f.at[slot, 1], recv_f.at[slot, core], ch, other)]
    peer_y = {5: rcopy(ybuf.at[5, bot], y_peer.at[0], send_y.at[0], recv_y.at[0], chip, other),
              6: rcopy(ybuf.at[6, bot], y_peer.at[1], send_y.at[1], recv_y.at[1], chip, other),
              7: rcopy(ybuf.at[7], y_own, send_y.at[2], recv_y.at[2], chip, other)}
    sums = {0: rcopy(s_out.at[0], s_in.at[1], send_s.at[0], recv_s.at[1], left, core),
            1: rcopy(s_out.at[1], s_in.at[0], send_s.at[1], recv_s.at[0], right, core)}

    for c in w_copies:
        c.start()
    barrier = pltpu.get_barrier_semaphore()
    for d in range(1, 2 * n_chip):
        pl.semaphore_signal(barrier, inc=1, device_id={"ep": lax.rem(ep + d, 2 * n_chip)}, device_id_type=MESH)
    pl.semaphore_wait(barrier, 2 * n_chip - 1)

    dispatch[1].start()
    dispatch[2].start()
    for c in gate:
        c.start()
    dispatch[5].start()
    dispatch[6].start()
    to_peer[7].start()
    hbuf[0] = h2_ref[...]
    gbuf[0] = ri_ref[...]

    dev_iota = lax.broadcasted_iota(jnp.int32, (2 * n_chip, 128), 0)

    def row_of(block, d):
        return jnp.sum(jnp.where(dev_iota == d, block, 0.0), axis=0, keepdims=True)

    def columns(rows):
        rows = rows + [jnp.zeros((128 - len(rows), 128), F32)]
        return jnp.concatenate(rows, axis=0).T

    def compute(u):
        for hf in range(2):
            rs = pl.ds(hf * hb, hb)
            ids = row_of(gbuf[u, 1, :, pl.ds(hf * hb, hb)], ep)
            cols = columns([(ids == float(e)).astype(F32) for e in range(e_local)])
            for e in range(e_local):
                keep = jnp.broadcast_to(cols[:, e:e + 1], (hb, 128)).astype(BF16)
                m_scr[e, rs, :] = keep
                for b in range(hidden // 128):
                    xm[rs, e * hidden + b * 128:e * hidden + (b + 1) * 128] = hbuf[u, rs, b * 128:(b + 1) * 128] * keep

        def up_tile(n, carry):
            cs = pl.ds(pl.multiple_of(n * 256, 256), 256)
            a = jnp.dot(xm[...], wg[:, cs], preferred_element_type=F32)
            b = jnp.dot(xm[...], wu[:, cs], preferred_element_type=F32)
            g = (a * (1.0 / (1.0 + jnp.exp(-a))) * b).astype(BF16)
            for e in range(e_local):
                for q in range(2):
                    gm[:, pl.ds(pl.multiple_of(n * 256, 256) + e * ff + q * 128, 128)] = g[:, q * 128:(q + 1) * 128] * m_scr[e]
            return carry

        lax.fori_loop(0, ff // 256, up_tile, 0)

        def down_tile(n, carry):
            cs = pl.ds(pl.multiple_of(n * 256, 256), 256)
            ybuf[u, :, cs] = jnp.dot(gm[...], wd[:, cs], preferred_element_type=F32).astype(BF16)
            return carry

        lax.fori_loop(0, hidden // 256, down_tile, 0)

    def gate_cols(u, lanes, devs):
        blk = gbuf[u, 0, :, lanes]
        return columns([row_of(blk, d) for d in devs])

    def wait_gate(u):
        if u == 7:
            gate[12].wait_recv()
        else:
            gate[2 * (u - 1)].wait_recv()
            gate[2 * (u - 1) + 1].wait_recv()

    def before(u):
        if u == 0:
            for c in w_copies:
                c.wait()
        if u == 1:
            for v in (1, 2):
                dispatch[v].wait_recv()
                dispatch[v + 2].start()
                to_peer[v].start()
        if u == 2:
            for v in (5, 6):
                dispatch[v].wait_recv()
                to_peer[v].start()
        if u == 3:
            for v in (3, 4):
                dispatch[v].wait_recv()
                to_peer[v].start()
        if u >= 1:
            to_peer[u].wait_recv()
            wait_gate(u)

    def after(u):
        if u in (1, 2):
            for c in near[u]:
                c.start()
        if u in (3, 4):
            for c in far[u]:
                c.start()
        if u in (5, 6, 7):
            peer_y[u].start()

    def unit(u, carry):
        for v in range(8):
            pl.when(u == v)(functools.partial(before, v))
        compute(u)
        for v in range(1, 8):
            pl.when(u == v)(functools.partial(after, v))
        return carry

    lax.fori_loop(0, 8, unit, 0)

    for slot, u, ch in ((0, 5, right), (1, 6, left)):
        peer_y[u].wait_recv()
        for co in range(2):
            rcopy(y_far.at[slot, co], y_far.at[slot, co], send_f.at[slot, co], recv_f.at[slot, co], ch, core).wait_recv()
        cols = gate_cols(u, pl.ds(0, 128), [ep, chip * 2 + other, ch * 2, ch * 2 + 1])
        s_out[slot] = (ybuf[u, top, :].astype(F32) * cols[:, 0:1] + y_peer[slot].astype(F32) * cols[:, 1:2]
                       + y_far[slot, 0].astype(F32) * cols[:, 2:3] + y_far[slot, 1].astype(F32) * cols[:, 3:4])
        sums[slot].start()

    peer_y[7].wait_recv()
    for hf, ch in ((0, right), (1, left)):
        rs = pl.ds(hf * hb, hb)
        for co in range(2):
            rcopy(y_near.at[hf, co], y_near.at[hf, co], send_n.at[hf, co], recv_n.at[hf, co], ch, core).wait_recv()
        cols = gate_cols(0, rs, [ep, chip * 2 + other, ch * 2, ch * 2 + 1])
        acc = (ybuf[0, rs, :].astype(F32) * cols[:, 0:1] + y_own[rs, :].astype(F32) * cols[:, 1:2]
               + y_near[hf, 0].astype(F32) * cols[:, 2:3] + y_near[hf, 1].astype(F32) * cols[:, 3:4])
        total = x1_ref[rs, :].astype(F32) + acc
        sums[1 - hf].wait_recv()
        out_ref[rs, :] = (total + s_in[hf]).astype(BF16)

    for group in (list(dispatch.values()), gate, list(to_peer.values()), near[1], near[2], far[3], far[4], list(peer_y.values()), list(sums.values())):
        for c in group:
            c.wait_send()


def moe(h2, ri, x1, w_gate, w_up, w_down, ep_size):
    n_tok, hidden = h2.shape
    e_local, _, ff = w_gate.shape
    hb = n_tok // 2
    dma = pltpu.SemaphoreType.DMA
    vmem = pl.BlockSpec(memory_space=pltpu.VMEM)
    hbm = pl.BlockSpec(memory_space=pl.ANY)
    return pl.pallas_call(
        functools.partial(moe_kernel, ep_size // 2),
        out_shape=jax.ShapeDtypeStruct((n_tok, hidden), BF16),
        in_specs=[vmem, vmem, vmem, hbm, hbm, hbm],
        out_specs=vmem,
        scratch_shapes=[
            pltpu.VMEM((e_local * hidden, ff), BF16), pltpu.VMEM((e_local * hidden, ff), BF16), pltpu.VMEM((e_local * ff, hidden), BF16),
            pltpu.VMEM((8, n_tok, hidden), BF16), pltpu.VMEM((8, 2, ep_size, n_tok), F32),
            pltpu.VMEM((n_tok, e_local * hidden), BF16), pltpu.VMEM((n_tok, e_local * ff), BF16), pltpu.VMEM((e_local, n_tok, 128), BF16),
            pltpu.VMEM((8, n_tok, hidden), BF16), pltpu.VMEM((2, 2, hb, hidden), BF16), pltpu.VMEM((2, 2, hb, hidden), BF16), pltpu.VMEM((2, hb, hidden), BF16), pltpu.VMEM((n_tok, hidden), BF16),
            pltpu.VMEM((2, hb, hidden), F32), pltpu.VMEM((2, hb, hidden), F32),
            dma((3,)), dma((8,)), dma((8,)), dma((8,)), dma((8,)), dma((15,)), dma((15,)), dma((2, 2)), dma((2, 2)), dma((2, 2)), dma((2, 2)), dma((3,)), dma((3,)), dma((2,)), dma((2,)),
        ],
        compiler_params=pltpu.CompilerParams(collective_id=0, has_side_effects=True),
        name="moe",
    )(h2, ri, x1, w_gate.reshape(e_local * hidden, ff), w_up.reshape(e_local * hidden, ff), w_down.reshape(e_local * ff, hidden))


def solution(mesh):
    ep_size = mesh.shape['ep']
    row_spec = P(('dp', 'ep'))
    replicated = P()
    expert_spec = P('ep')
    in_specs = (row_spec,) * 5 + (replicated,) * 9 + (expert_spec,) * 3

    def device_step(x_in, k_cache, v_cache, cache_len, topk_idx, ln_attn, w_q, w_k, w_v, q_norm, k_norm, w_o, ln_moe, w_router, w_gate, w_up, w_down):
        x1, h2, ri, k_new, v_new = attention(x_in, k_cache, v_cache, cache_len, topk_idx, ln_attn, w_q, w_k, w_v, q_norm, k_norm, w_o, ln_moe, w_router, ep_size)
        return moe(h2, ri, x1, w_gate, w_up, w_down, ep_size), k_new, v_new

    return jax.shard_map(device_step, mesh=mesh, in_specs=in_specs, out_specs=(row_spec,) * 3, check_vma=False)
```

```python
import functools

import jax
import jax.numpy as jnp
import numpy as np
from jax import lax
from jax.experimental import pallas as pl
from jax.experimental.pallas import tpu as pltpu
from jax.sharding import PartitionSpec as P

ROPE_BASE = 1000000.0
NORM_EPS = 1e-6
F32 = jnp.float32
BF16 = jnp.bfloat16
MESH = pl.DeviceIdType.MESH


def sublane_sums(parts):
    row = lax.broadcasted_iota(jnp.int32, parts[0].shape, 0)
    for d in (1, 2, 4):
        low = (row & d) == 0
        parts = [jnp.where(low, a, b) + pltpu.roll(jnp.where(low, b, a), d, 0) for a, b in zip(parts[0::2], parts[1::2])]
    return parts[0]


def attn_kernel(freq_ref, x_ref, len_ref, topk_ref, lna_ref, qn_ref, kn_ref, lnm_ref, wr_ref, wq_hbm, wk_hbm, wv_hbm, wo_hbm, kc_hbm, vc_hbm,
                x1_ref, h2_ref, ri_ref, kco_hbm, vco_hbm,
                wq_scr, wk_scr, wv_scr, wo_scr, kbuf, vbuf, h_scr, cos_scr, sin_scr, qg_scr, kg_scr, len_scr, q_scr, kn_scr, vn_scr, s_scr, o_scr,
                w_sem, kin_sem, vin_sem, kout_sem, vout_sem):
    n_tok = x_ref.shape[0]
    n_head, n_slots, head_dim, _ = kbuf.shape
    half = head_dim // 2
    n_lt = n_tok // 128
    early = 1
    ahead = 4

    w_copies = [pltpu.make_async_copy(src, dst, w_sem.at[i]) for i, (src, dst) in enumerate(((wk_hbm, wk_scr), (wv_hbm, wv_scr), (wq_hbm, wq_scr), (wo_hbm, wo_scr)))]

    def reads(g):
        return (pltpu.make_async_copy(kc_hbm.at[:, g], kbuf.at[g], kin_sem.at[g]), pltpu.make_async_copy(vc_hbm.at[:, g], vbuf.at[g], vin_sem.at[g]))

    def writes(g):
        return (pltpu.make_async_copy(kbuf.at[g], kco_hbm.at[:, g], kout_sem.at[g]), pltpu.make_async_copy(vbuf.at[g], vco_hbm.at[:, g], vout_sem.at[g]))

    for c in w_copies[:3]:
        c.start()
    for g in range(early):
        for c in reads(g):
            c.start()

    xf = x_ref[...].astype(F32)
    ms = jnp.mean(xf * xf, axis=1, keepdims=True)
    h_scr[...] = (xf * lax.rsqrt(ms + NORM_EPS) * lna_ref[...].astype(F32)[None, :]).astype(BF16)
    lens = len_ref[...].astype(F32)
    angles = jnp.concatenate([freq_ref[...]] * n_lt, axis=1) * lens
    cos_scr[...] = jnp.cos(angles)
    sin_scr[...] = jnp.sin(angles)
    for src, dst in ((qn_ref, qg_scr), (kn_ref, kg_scr)):
        row = src[...].astype(F32)
        dst[...] = jnp.broadcast_to(jnp.concatenate([row, row], axis=1), (128, 128)).T[:head_dim]
    len_scr[...] = jnp.broadcast_to(lens, (16, n_tok)).astype(BF16)

    def head_rope(block, gain_scr):
        ms = jnp.mean(block * block, axis=0, keepdims=True)
        gain = jnp.concatenate([gain_scr[...]] * n_lt, axis=1)
        block = block * lax.rsqrt(ms + NORM_EPS) * gain
        lo, hi = block[:half], block[half:]
        cosv, sinv = cos_scr[...], sin_scr[...]
        return jnp.concatenate([lo * cosv - hi * sinv, hi * cosv + lo * sinv], axis=0).astype(BF16)

    per = 256 // head_dim
    for c in w_copies[:3]:
        c.wait()
    for g in range(early, ahead):
        for c in reads(g):
            c.start()
    w_copies[3].start()

    def project(w_scr, i):
        cols = pl.ds(pl.multiple_of(i * 256, 256), 256)
        return jnp.dot(h_scr[...], w_scr[:, cols], preferred_element_type=F32).T

    def kv_proj(i, carry):
        k_t = project(wk_scr, i)
        v_t = project(wv_scr, i)
        for j in range(per):
            kn_scr[i * per + j] = head_rope(k_t[j * head_dim:(j + 1) * head_dim], kg_scr)
            vn_scr[i * per + j] = v_t[j * head_dim:(j + 1) * head_dim].astype(BF16)
        return carry

    def q_proj(i, carry):
        q_t = project(wq_scr, i)
        for j in range(per):
            q_scr[i * per + j] = head_rope(q_t[j * head_dim:(j + 1) * head_dim], qg_scr).astype(F32)
        return carry

    lax.fori_loop(0, n_head // per, kv_proj, 0, unroll=True)
    lax.fori_loop(0, 2 * n_head // per, q_proj, 0, unroll=True)

    tiles = [pl.ds(r * 16, 16) for r in range(head_dim // 16)]

    def head(g, carry):
        @pl.when(g + ahead < n_head)
        def _():
            for c in reads(g + ahead):
                c.start()

        for c in reads(g):
            c.wait()

        for lt in range(n_lt):
            lanes = pl.ds(lt * 128, 128)

            def score_block(i, carry):
                parts = [[], []]
                for si in range(8):
                    s = i * 8 + si
                    hit = len_scr[:, lanes] == s.astype(F32).astype(BF16)
                    accs = [None, None]
                    for t in tiles:
                        kb = kbuf[g, s, t, lanes]
                        kbuf[g, s, t, lanes] = jnp.where(hit, kn_scr[g, t, lanes], kb)
                        kf = kb.astype(F32)
                        for j in range(2):
                            prod = kf * q_scr[2 * g + j, t, lanes]
                            accs[j] = prod if accs[j] is None else accs[j] + prod
                    for j in range(2):
                        parts[j].append(accs[j][:8] + accs[j][8:])
                for j in range(2):
                    s_scr[j, pl.ds(pl.multiple_of(i * 8, 8), 8), lanes] = sublane_sums(parts[j])
                return carry

            lax.fori_loop(0, n_slots // 8, score_block, 0)
            slot = lax.broadcasted_iota(jnp.int32, (n_slots, 128), 0)
            len_row = len_ref[:, lanes]
            kn = kn_scr[g, :, lanes].astype(F32)
            vn = vn_scr[g, :, lanes].astype(F32)
            accs = []
            for j in range(2):
                fresh = jnp.sum(kn * q_scr[2 * g + j, :, lanes], axis=0, keepdims=True)
                sc = jnp.where(slot == len_row, fresh, s_scr[j, :, lanes]) * (head_dim ** -0.5)
                sc = jnp.where(slot <= len_row, sc, -1e30)
                ex = jnp.exp(sc - jnp.max(sc, axis=0, keepdims=True))
                pr = (ex / jnp.sum(ex, axis=0, keepdims=True)).astype(BF16).astype(F32)
                accs.append(jnp.sum(jnp.where(slot == len_row, pr, 0.0), axis=0, keepdims=True) * vn)
                s_scr[j, :, lanes] = jnp.where(slot == len_row, 0.0, pr)

            def value_block(i, accs):
                accs = [[a[r * 16:(r + 1) * 16] for r in range(len(tiles))] for a in accs]
                prob = [s_scr[j, pl.ds(pl.multiple_of(i * 8, 8), 8), lanes] for j in range(2)]
                for si in range(8):
                    s = i * 8 + si
                    hit = len_scr[:, lanes] == s.astype(F32).astype(BF16)
                    for r, t in enumerate(tiles):
                        vb = vbuf[g, s, t, lanes]
                        vbuf[g, s, t, lanes] = jnp.where(hit, vn_scr[g, t, lanes], vb)
                        vf = vb.astype(F32)
                        for j in range(2):
                            accs[j][r] = accs[j][r] + prob[j][si:si + 1] * vf
                return tuple(jnp.concatenate(a, axis=0) for a in accs)

            accs = lax.fori_loop(0, n_slots // 8, value_block, tuple(accs))
            o_scr[pl.ds(lt * 128, 128), pl.ds(pl.multiple_of(g * 128, 128), 128)] = jnp.concatenate(accs, axis=0).T.astype(BF16)
        for c in writes(g):
            c.start()
        return carry

    lax.fori_loop(0, n_head, head, 0)

    w_copies[3].wait()
    x1 = (x_ref[...].astype(F32) + jnp.dot(o_scr[...], wo_scr[...], preferred_element_type=F32)).astype(BF16)
    x1_ref[...] = x1
    xf = x1.astype(F32)
    ms = jnp.mean(xf * xf, axis=1, keepdims=True)
    h2 = (xf * lax.rsqrt(ms + NORM_EPS) * lnm_ref[...].astype(F32)[None, :]).astype(BF16)
    h2_ref[...] = h2
    logits = lax.dot_general(wr_ref[...], h2, (((1,), (1,)), ((), ())), preferred_element_type=F32)
    top_k = topk_ref.shape[0]
    n_exp = wr_ref.shape[0]
    n_dev = ri_ref.shape[1]
    e_local = n_exp // n_dev
    exp_id = lax.broadcasted_iota(jnp.int32, (n_exp, n_tok), 0)
    picked = [jnp.sum(jnp.where(exp_id == topk_ref[pl.ds(k, 1), :], logits, 0.0), axis=0, keepdims=True) for k in range(top_k)]
    picked = jnp.concatenate(picked, axis=0)
    ex = jnp.exp(picked - jnp.max(picked, axis=0, keepdims=True))
    gate = ex / jnp.sum(ex, axis=0, keepdims=True)
    dev_id = lax.broadcasted_iota(jnp.int32, (n_dev, n_tok), 0)
    r_dev = jnp.zeros((n_dev, n_tok), F32)
    i_dev = jnp.zeros((n_dev, n_tok), F32)
    for k in range(top_k):
        idx = topk_ref[pl.ds(k, 1), :]
        dev = idx // e_local
        mine = dev_id == dev
        r_dev = r_dev + jnp.where(mine, gate[k:k + 1], 0.0)
        i_dev = i_dev + jnp.where(mine, (idx - dev * e_local).astype(F32), 0.0)
    ri_ref[0] = r_dev
    ri_ref[1] = i_dev

    def drain(g, carry):
        for c in writes(g):
            c.wait()
        return carry

    lax.fori_loop(0, n_head, drain, 0)


def attention(x_in, k_cache, v_cache, cache_len, topk_idx, ln_attn, w_q, w_k, w_v, q_norm, k_norm, w_o, ln_moe, w_router, ep_size):
    n_tok, hidden = x_in.shape
    _, n_slots, kv_heads, head_dim = k_cache.shape
    freq = np.float32(ROPE_BASE) ** (-np.arange(head_dim // 2, dtype=np.float32) * np.float32(2.0) / np.float32(head_dim))
    freq = jnp.asarray(np.ascontiguousarray(np.broadcast_to(freq[:, None], (head_dim // 2, 128))), F32)
    kt = k_cache.transpose(1, 2, 3, 0)
    vt = v_cache.transpose(1, 2, 3, 0)
    vmem = pl.BlockSpec(memory_space=pltpu.VMEM)
    hbm = pl.BlockSpec(memory_space=pl.ANY)
    dma = pltpu.SemaphoreType.DMA
    out = pl.pallas_call(
        attn_kernel,
        in_specs=[vmem] * 9 + [hbm] * 6,
        out_specs=[vmem, vmem, vmem, hbm, hbm],
        out_shape=[
            jax.ShapeDtypeStruct((n_tok, hidden), BF16), jax.ShapeDtypeStruct((n_tok, hidden), BF16), jax.ShapeDtypeStruct((2, ep_size, n_tok), F32),
            jax.ShapeDtypeStruct(kt.shape, BF16), jax.ShapeDtypeStruct(vt.shape, BF16),
        ],
        scratch_shapes=[
            pltpu.VMEM(w_q.shape, BF16), pltpu.VMEM(w_k.shape, BF16), pltpu.VMEM(w_v.shape, BF16), pltpu.VMEM(w_o.shape, BF16),
            pltpu.VMEM((kv_heads, n_slots, head_dim, n_tok), BF16), pltpu.VMEM((kv_heads, n_slots, head_dim, n_tok), BF16),
            pltpu.VMEM((n_tok, hidden), BF16), pltpu.VMEM((head_dim // 2, n_tok), F32), pltpu.VMEM((head_dim // 2, n_tok), F32),
            pltpu.VMEM((head_dim, 128), F32), pltpu.VMEM((head_dim, 128), F32), pltpu.VMEM((16, n_tok), BF16),
            pltpu.VMEM((2 * kv_heads, head_dim, n_tok), F32), pltpu.VMEM((kv_heads, head_dim, n_tok), BF16), pltpu.VMEM((kv_heads, head_dim, n_tok), BF16),
            pltpu.VMEM((2, n_slots, n_tok), F32), pltpu.VMEM((n_tok, w_q.shape[1]), BF16),
            dma((4,)), dma((kv_heads,)), dma((kv_heads,)), dma((kv_heads,)), dma((kv_heads,)),
        ],
        name="attend",
    )(freq, x_in, cache_len.reshape(1, n_tok), topk_idx.T, ln_attn, q_norm.reshape(1, head_dim), k_norm.reshape(1, head_dim),
      ln_moe, w_router.T, w_q, w_k, w_v, w_o, kt, vt)
    x1, h2, ri, kto, vto = out
    return x1, h2, ri, kto.transpose(3, 0, 1, 2), vto.transpose(3, 0, 1, 2)


def moe_kernel(n_chip, h2_ref, ri_ref, x1_ref, wg_hbm, wu_hbm, wd_hbm, out_ref,
               wg, wu, wd, hbuf, gsrc, gbuf, xm, gm, m_scr, ybuf, y_near, y_far, y_peer, y_own, s_out, s_in, acc_scr,
               w_sem, send_h, recv_h, send_p, recv_p, send_g, recv_g, send_n, recv_n, send_f, recv_f, send_y, recv_y, send_s, recv_s):
    ep = lax.axis_index("ep")
    core = lax.rem(ep, 2)
    chip = ep // 2
    right = lax.rem(chip + 1, n_chip)
    left = lax.rem(chip + n_chip - 1, n_chip)
    opp = lax.rem(chip + 2, n_chip)
    other = 1 - core
    n_tok, hidden = h2_ref.shape
    hb = n_tok // 2
    qb = hb // 2
    e_local = wg.shape[0] // hidden
    ff = wg.shape[1]

    def dev(ch, co):
        return {"ep": ch * 2 + co}

    def rcopy(src, dst, ssem, rsem, ch, co):
        return pltpu.make_async_remote_copy(src_ref=src, dst_ref=dst, send_sem=ssem, recv_sem=rsem, device_id=dev(ch, co), device_id_type=MESH)

    top = pl.ds(0, hb)
    bot = pl.ds(hb, hb)

    w_copies = [pltpu.make_async_copy(wg_hbm, wg, w_sem.at[0]), pltpu.make_async_copy(wu_hbm, wu, w_sem.at[1]), pltpu.make_async_copy(wd_hbm, wd, w_sem.at[2])]

    dispatch = {
        1: rcopy(h2_ref.at[top], hbuf.at[1, top], send_h.at[1], recv_h.at[1], right, core),
        2: rcopy(h2_ref.at[bot], hbuf.at[2, top], send_h.at[2], recv_h.at[2], left, core),
        5: rcopy(h2_ref.at[bot], hbuf.at[5, top], send_h.at[5], recv_h.at[5], right, core),
        6: rcopy(h2_ref.at[top], hbuf.at[6, top], send_h.at[6], recv_h.at[6], left, core),
        3: rcopy(hbuf.at[1, top], hbuf.at[3, top], send_h.at[3], recv_h.at[3], right, core),
        4: rcopy(hbuf.at[2, top], hbuf.at[4, top], send_h.at[4], recv_h.at[4], left, core),
    }
    to_peer = {u: rcopy(hbuf.at[u, top], hbuf.at[u, bot], send_p.at[u], recv_p.at[u], chip, other) for u in range(1, 7)}
    to_peer[7] = rcopy(h2_ref, hbuf.at[7], send_p.at[7], recv_p.at[7], chip, other)
    gate = {}
    for rel, ch in ((0, chip), (1, right), (2, opp), (3, left)):
        for q, co in ((0, core), (1, other)):
            if rel or q:
                gate[2 * rel + q] = rcopy(ri_ref, gsrc.at[2 * rel + q], send_g.at[2 * rel + q], recv_g.at[2 * rel + q], ch, co)

    near = {}
    far = {}
    for u, ch, slot in ((1, left, 0), (2, right, 1)):
        near[u] = [rcopy(ybuf.at[u, top], y_near.at[slot, core], send_n.at[slot, 0], recv_n.at[slot, core], ch, core),
                   rcopy(ybuf.at[u, bot], y_near.at[slot, core], send_n.at[slot, 1], recv_n.at[slot, core], ch, other)]
    for u, ch, slot in ((3, right, 1), (4, left, 0)):
        far[u] = []
        for p in range(2):
            rows = pl.ds(p * qb, qb)
            far[u].append(rcopy(ybuf.at[u, rows], y_far.at[slot, core, rows], send_f.at[slot, p, 0], recv_f.at[slot, core, p], ch, core))
            far[u].append(rcopy(ybuf.at[u, pl.ds(hb + p * qb, qb)], y_far.at[slot, core, rows], send_f.at[slot, p, 1], recv_f.at[slot, core, p], ch, other))
    peer_y = {5: rcopy(ybuf.at[5, bot], y_peer.at[0], send_y.at[0], recv_y.at[0], chip, other),
              6: rcopy(ybuf.at[6, bot], y_peer.at[1], send_y.at[1], recv_y.at[1], chip, other),
              7: rcopy(ybuf.at[7], y_own, send_y.at[2], recv_y.at[2], chip, other)}
    sums = {}
    for p in range(2):
        rows = pl.ds(p * qb, qb)
        sums[0, p] = rcopy(s_out.at[0, rows], s_in.at[1, rows], send_s.at[0, p], recv_s.at[1, p], left, core)
        sums[1, p] = rcopy(s_out.at[1, rows], s_in.at[0, rows], send_s.at[1, p], recv_s.at[0, p], right, core)

    for c in w_copies:
        c.start()
    barrier = pltpu.get_barrier_semaphore()
    for d in range(1, 2 * n_chip):
        pl.semaphore_signal(barrier, inc=1, device_id={"ep": lax.rem(ep + d, 2 * n_chip)}, device_id_type=MESH)
    pl.semaphore_wait(barrier, 2 * n_chip - 1)

    dispatch[1].start()
    dispatch[2].start()
    for c in gate.values():
        c.start()
    dispatch[5].start()
    dispatch[6].start()
    to_peer[7].start()
    hbuf[0] = h2_ref[...]
    gbuf[0] = ri_ref[...]

    dev_iota = lax.broadcasted_iota(jnp.int32, (2 * n_chip, 128), 0)

    def row_of(block, d):
        return jnp.sum(jnp.where(dev_iota == d, block, 0.0), axis=0, keepdims=True)

    def columns(rows):
        rows = rows + [jnp.zeros((128 - len(rows), 128), F32)]
        return jnp.concatenate(rows, axis=0).T

    def compute(u):
        for hf in range(2):
            rs = pl.ds(hf * hb, hb)
            ids = row_of(gbuf[u, 1, :, pl.ds(hf * hb, hb)], ep)
            cols = columns([(ids == float(e)).astype(F32) for e in range(e_local)])
            for e in range(e_local):
                keep = jnp.broadcast_to(cols[:, e:e + 1], (hb, 128)).astype(BF16)
                m_scr[e, rs, :] = keep
                for b in range(hidden // 128):
                    xm[rs, e * hidden + b * 128:e * hidden + (b + 1) * 128] = hbuf[u, rs, b * 128:(b + 1) * 128] * keep

        def up_tile(n, carry):
            cs = pl.ds(pl.multiple_of(n * 256, 256), 256)
            a = jnp.dot(xm[...], wg[:, cs], preferred_element_type=F32)
            b = jnp.dot(xm[...], wu[:, cs], preferred_element_type=F32)
            g = (a * (1.0 / (1.0 + jnp.exp(-a))) * b).astype(BF16)
            for e in range(e_local):
                for q in range(2):
                    gm[:, pl.ds(pl.multiple_of(n * 256, 256) + e * ff + q * 128, 128)] = g[:, q * 128:(q + 1) * 128] * m_scr[e]
            return carry

        lax.fori_loop(0, ff // 256, up_tile, 0)

        def down_tile(n, carry):
            cs = pl.ds(pl.multiple_of(n * 256, 256), 256)
            ybuf[u, :, cs] = jnp.dot(gm[...], wd[:, cs], preferred_element_type=F32).astype(BF16)
            return carry

        lax.fori_loop(0, hidden // 256, down_tile, 0)

    def gate_cols(u, lanes, devs):
        blk = gbuf[u, 0, :, lanes]
        return columns([row_of(blk, d) for d in devs])

    def take_gate(u):
        if u == 7:
            gate[1].wait_recv()
            gbuf[7] = gsrc[1]
            return
        rel, hf = ((1, 0), (3, 1), (2, 0), (2, 1), (1, 1), (3, 0))[u - 1]
        for q in range(2):
            if u in (1, 2, 3):
                gate[2 * rel + q].wait_recv()
            gbuf[u, :, :, pl.ds(q * hb, hb)] = gsrc[2 * rel + q, :, :, pl.ds(hf * hb, hb)]

    def send_sums():
        for slot, u in ((0, 5), (1, 6)):
            peer_y[u].wait_recv()
        for p in range(2):
            rows = pl.ds(p * qb, qb)
            for slot, u, ch in ((0, 5, right), (1, 6, left)):
                for co in range(2):
                    piece = y_far.at[slot, co, rows]
                    rcopy(piece, piece, send_f.at[slot, p, co], recv_f.at[slot, co, p], ch, core).wait_recv()
                cols = gate_cols(u, pl.ds(0, 128), [ep, chip * 2 + other, ch * 2, ch * 2 + 1])[p * qb:(p + 1) * qb]
                s_out[slot, rows] = (ybuf[u, rows, :].astype(F32) * cols[:, 0:1] + y_peer[slot, rows].astype(F32) * cols[:, 1:2]
                                     + y_far[slot, 0, rows].astype(F32) * cols[:, 2:3] + y_far[slot, 1, rows].astype(F32) * cols[:, 3:4])
                sums[slot, p].start()

    def before(u):
        if u == 0:
            for c in w_copies:
                c.wait()
        if u == 1:
            for v in (1, 2):
                dispatch[v].wait_recv()
                dispatch[v + 2].start()
                to_peer[v].start()
        if u == 2:
            for v in (5, 6):
                dispatch[v].wait_recv()
                to_peer[v].start()
        if u == 3:
            for v in (3, 4):
                dispatch[v].wait_recv()
                to_peer[v].start()
        if u == 7:
            send_sums()
        if u >= 1:
            to_peer[u].wait_recv()
            take_gate(u)

    def after(u):
        if u in (1, 2):
            for c in near[u]:
                c.start()
        if u in (3, 4):
            for c in far[u]:
                c.start()
        if u in (5, 6, 7):
            peer_y[u].start()

    def unit(u, carry):
        for v in range(8):
            pl.when(u == v)(functools.partial(before, v))
        compute(u)
        for v in range(1, 8):
            pl.when(u == v)(functools.partial(after, v))
        return carry

    lax.fori_loop(0, 8, unit, 0)

    peer_y[7].wait_recv()
    for hf, ch in ((0, right), (1, left)):
        rs = pl.ds(hf * hb, hb)
        for co in range(2):
            rcopy(y_near.at[hf, co], y_near.at[hf, co], send_n.at[hf, co], recv_n.at[hf, co], ch, core).wait_recv()
        cols = gate_cols(0, rs, [ep, chip * 2 + other, ch * 2, ch * 2 + 1])
        acc_scr[rs, :] = x1_ref[rs, :].astype(F32) + (
            ybuf[0, rs, :].astype(F32) * cols[:, 0:1] + y_own[rs, :].astype(F32) * cols[:, 1:2]
            + y_near[hf, 0].astype(F32) * cols[:, 2:3] + y_near[hf, 1].astype(F32) * cols[:, 3:4])
    for p in range(2):
        for hf in range(2):
            rows = pl.ds(p * qb, qb)
            rs = pl.ds(hf * hb + p * qb, qb)
            sums[1 - hf, p].wait_recv()
            out_ref[rs, :] = (acc_scr[rs, :] + s_in[hf, rows]).astype(BF16)

    for group in (list(dispatch.values()), list(gate.values()), list(to_peer.values()), near[1], near[2], far[3], far[4], list(peer_y.values()), list(sums.values())):
        for c in group:
            c.wait_send()


def moe(h2, ri, x1, w_gate, w_up, w_down, ep_size):
    n_tok, hidden = h2.shape
    e_local, _, ff = w_gate.shape
    hb = n_tok // 2
    dma = pltpu.SemaphoreType.DMA
    vmem = pl.BlockSpec(memory_space=pltpu.VMEM)
    hbm = pl.BlockSpec(memory_space=pl.ANY)
    return pl.pallas_call(
        functools.partial(moe_kernel, ep_size // 2),
        out_shape=jax.ShapeDtypeStruct((n_tok, hidden), BF16),
        in_specs=[vmem, vmem, vmem, hbm, hbm, hbm],
        out_specs=vmem,
        scratch_shapes=[
            pltpu.VMEM((e_local * hidden, ff), BF16), pltpu.VMEM((e_local * hidden, ff), BF16), pltpu.VMEM((e_local * ff, hidden), BF16),
            pltpu.VMEM((8, n_tok, hidden), BF16), pltpu.VMEM((8, 2, ep_size, n_tok), F32), pltpu.VMEM((8, 2, ep_size, n_tok), F32),
            pltpu.VMEM((n_tok, e_local * hidden), BF16), pltpu.VMEM((n_tok, e_local * ff), BF16), pltpu.VMEM((e_local, n_tok, 128), BF16),
            pltpu.VMEM((8, n_tok, hidden), BF16), pltpu.VMEM((2, 2, hb, hidden), BF16), pltpu.VMEM((2, 2, hb, hidden), BF16), pltpu.VMEM((2, hb, hidden), BF16), pltpu.VMEM((n_tok, hidden), BF16),
            pltpu.VMEM((2, hb, hidden), F32), pltpu.VMEM((2, hb, hidden), F32), pltpu.VMEM((n_tok, hidden), F32),
            dma((3,)), dma((8,)), dma((8,)), dma((8,)), dma((8,)), dma((8,)), dma((8,)), dma((2, 2)), dma((2, 2)), dma((2, 2, 2)), dma((2, 2, 2)), dma((3,)), dma((3,)), dma((2, 2)), dma((2, 2)),
        ],
        compiler_params=pltpu.CompilerParams(collective_id=0, has_side_effects=True),
        name="moe",
    )(h2, ri, x1, w_gate.reshape(e_local * hidden, ff), w_up.reshape(e_local * hidden, ff), w_down.reshape(e_local * ff, hidden))


def solution(mesh):
    ep_size = mesh.shape['ep']
    row_spec = P(('dp', 'ep'))
    replicated = P()
    expert_spec = P('ep')
    in_specs = (row_spec,) * 5 + (replicated,) * 9 + (expert_spec,) * 3

    def device_step(x_in, k_cache, v_cache, cache_len, topk_idx, ln_attn, w_q, w_k, w_v, q_norm, k_norm, w_o, ln_moe, w_router, w_gate, w_up, w_down):
        x1, h2, ri, k_new, v_new = attention(x_in, k_cache, v_cache, cache_len, topk_idx, ln_attn, w_q, w_k, w_v, q_norm, k_norm, w_o, ln_moe, w_router, ep_size)
        return moe(h2, ri, x1, w_gate, w_up, w_down, ep_size), k_new, v_new

    return jax.shard_map(device_step, mesh=mesh, in_specs=in_specs, out_specs=(row_spec,) * 3, check_vma=False)
```

```python
import functools

import jax
import jax.numpy as jnp
import numpy as np
from jax import lax
from jax.experimental import pallas as pl
from jax.experimental.pallas import tpu as pltpu
from jax.sharding import PartitionSpec as P

ROPE_BASE = 1000000.0
NORM_EPS = 1e-6
F32 = jnp.float32
BF16 = jnp.bfloat16
MESH = pl.DeviceIdType.MESH


def sublane_sums(parts):
    row = lax.broadcasted_iota(jnp.int32, parts[0].shape, 0)
    for d in (1, 2, 4):
        low = (row & d) == 0
        parts = [jnp.where(low, a, b) + pltpu.roll(jnp.where(low, b, a), d, 0) for a, b in zip(parts[0::2], parts[1::2])]
    return parts[0]


def attn_body(small_copies, freq_ref, x_ref, len_ref, topk_ref, lna_ref, qn_ref, kn_ref, lnm_ref, wr_ref, wq_hbm, wk_hbm, wv_hbm, wo_hbm, kc_hbm, vc_hbm,
                x1_ref, h2_ref, ri_ref, kco_hbm, vco_hbm,
                wq_scr, wk_scr, wv_scr, wo_scr, kbuf, vbuf, h_scr, cos_scr, sin_scr, qg_scr, kg_scr, len_scr, q_scr, kn_scr, vn_scr, s_scr, o_scr,
                w_sem, kin_sem, vin_sem, kout_sem, vout_sem):
    n_tok = x_ref.shape[0]
    n_head, n_slots, head_dim, _ = kbuf.shape
    half = head_dim // 2
    n_lt = n_tok // 128
    early = 1
    ahead = 4

    w_copies = [pltpu.make_async_copy(src, dst, w_sem.at[i]) for i, (src, dst) in enumerate(((wk_hbm, wk_scr), (wv_hbm, wv_scr), (wq_hbm, wq_scr), (wo_hbm, wo_scr)))]

    def reads(g):
        return (pltpu.make_async_copy(kc_hbm.at[:, g], kbuf.at[g], kin_sem.at[g]), pltpu.make_async_copy(vc_hbm.at[:, g], vbuf.at[g], vin_sem.at[g]))

    def writes(g):
        return (pltpu.make_async_copy(kbuf.at[g], kco_hbm.at[:, g], kout_sem.at[g]), pltpu.make_async_copy(vbuf.at[g], vco_hbm.at[:, g], vout_sem.at[g]))

    for c in small_copies + w_copies[:3]:
        c.start()
    for g in range(early):
        for c in reads(g):
            c.start()
    for c in small_copies:
        c.wait()

    xf = x_ref[...].astype(F32)
    ms = jnp.mean(xf * xf, axis=1, keepdims=True)
    h_scr[...] = (xf * lax.rsqrt(ms + NORM_EPS) * lna_ref[...].astype(F32)[None, :]).astype(BF16)
    lens = len_ref[...].astype(F32)
    angles = jnp.concatenate([freq_ref[...]] * n_lt, axis=1) * lens
    cos_scr[...] = jnp.cos(angles)
    sin_scr[...] = jnp.sin(angles)
    for src, dst in ((qn_ref, qg_scr), (kn_ref, kg_scr)):
        row = src[...].astype(F32)
        dst[...] = jnp.broadcast_to(jnp.concatenate([row, row], axis=1), (128, 128)).T[:head_dim]
    len_scr[...] = jnp.broadcast_to(lens, (16, n_tok)).astype(BF16)

    def head_rope(block, gain_scr):
        ms = jnp.mean(block * block, axis=0, keepdims=True)
        gain = jnp.concatenate([gain_scr[...]] * n_lt, axis=1)
        block = block * lax.rsqrt(ms + NORM_EPS) * gain
        lo, hi = block[:half], block[half:]
        cosv, sinv = cos_scr[...], sin_scr[...]
        return jnp.concatenate([lo * cosv - hi * sinv, hi * cosv + lo * sinv], axis=0).astype(BF16)

    per = 256 // head_dim
    for c in w_copies[:3]:
        c.wait()
    for g in range(early, ahead):
        for c in reads(g):
            c.start()
    w_copies[3].start()

    def project(w_scr, i):
        cols = pl.ds(pl.multiple_of(i * 256, 256), 256)
        return jnp.dot(h_scr[...], w_scr[:, cols], preferred_element_type=F32).T

    def kv_proj(i, carry):
        k_t = project(wk_scr, i)
        v_t = project(wv_scr, i)
        for j in range(per):
            kn_scr[i * per + j] = head_rope(k_t[j * head_dim:(j + 1) * head_dim], kg_scr)
            vn_scr[i * per + j] = v_t[j * head_dim:(j + 1) * head_dim].astype(BF16)
        return carry

    def q_proj(i, carry):
        q_t = project(wq_scr, i)
        for j in range(per):
            q_scr[i * per + j] = head_rope(q_t[j * head_dim:(j + 1) * head_dim], qg_scr).astype(F32)
        return carry

    lax.fori_loop(0, n_head // per, kv_proj, 0, unroll=True)
    lax.fori_loop(0, 2 * n_head // per, q_proj, 0, unroll=True)

    tiles = [pl.ds(r * 16, 16) for r in range(head_dim // 16)]

    def head(g, carry):
        @pl.when(g + ahead < n_head)
        def _():
            for c in reads(g + ahead):
                c.start()

        for c in reads(g):
            c.wait()

        for lt in range(n_lt):
            lanes = pl.ds(lt * 128, 128)

            def score_block(i, carry):
                parts = [[], []]
                for si in range(8):
                    s = i * 8 + si
                    hit = len_scr[:, lanes] == s.astype(F32).astype(BF16)
                    accs = [None, None]
                    for t in tiles:
                        kb = kbuf[g, s, t, lanes]
                        kbuf[g, s, t, lanes] = jnp.where(hit, kn_scr[g, t, lanes], kb)
                        kf = kb.astype(F32)
                        for j in range(2):
                            prod = kf * q_scr[2 * g + j, t, lanes]
                            accs[j] = prod if accs[j] is None else accs[j] + prod
                    for j in range(2):
                        parts[j].append(accs[j][:8] + accs[j][8:])
                for j in range(2):
                    s_scr[j, pl.ds(pl.multiple_of(i * 8, 8), 8), lanes] = sublane_sums(parts[j])
                return carry

            lax.fori_loop(0, n_slots // 8, score_block, 0)
            slot = lax.broadcasted_iota(jnp.int32, (n_slots, 128), 0)
            len_row = len_ref[:, lanes]
            kn = kn_scr[g, :, lanes].astype(F32)
            vn = vn_scr[g, :, lanes].astype(F32)
            accs = []
            for j in range(2):
                fresh = jnp.sum(kn * q_scr[2 * g + j, :, lanes], axis=0, keepdims=True)
                sc = jnp.where(slot == len_row, fresh, s_scr[j, :, lanes]) * (head_dim ** -0.5)
                sc = jnp.where(slot <= len_row, sc, -1e30)
                ex = jnp.exp(sc - jnp.max(sc, axis=0, keepdims=True))
                pr = (ex / jnp.sum(ex, axis=0, keepdims=True)).astype(BF16).astype(F32)
                accs.append(jnp.sum(jnp.where(slot == len_row, pr, 0.0), axis=0, keepdims=True) * vn)
                s_scr[j, :, lanes] = jnp.where(slot == len_row, 0.0, pr)

            def value_block(i, accs):
                accs = [[a[r * 16:(r + 1) * 16] for r in range(len(tiles))] for a in accs]
                prob = [s_scr[j, pl.ds(pl.multiple_of(i * 8, 8), 8), lanes] for j in range(2)]
                for si in range(8):
                    s = i * 8 + si
                    hit = len_scr[:, lanes] == s.astype(F32).astype(BF16)
                    for r, t in enumerate(tiles):
                        vb = vbuf[g, s, t, lanes]
                        vbuf[g, s, t, lanes] = jnp.where(hit, vn_scr[g, t, lanes], vb)
                        vf = vb.astype(F32)
                        for j in range(2):
                            accs[j][r] = accs[j][r] + prob[j][si:si + 1] * vf
                return tuple(jnp.concatenate(a, axis=0) for a in accs)

            accs = lax.fori_loop(0, n_slots // 8, value_block, tuple(accs))
            o_scr[pl.ds(lt * 128, 128), pl.ds(pl.multiple_of(g * 128, 128), 128)] = jnp.concatenate(accs, axis=0).T.astype(BF16)
        for c in writes(g):
            c.start()
        return carry

    lax.fori_loop(0, n_head, head, 0)

    w_copies[3].wait()
    x1 = (x_ref[...].astype(F32) + jnp.dot(o_scr[...], wo_scr[...], preferred_element_type=F32)).astype(BF16)
    x1_ref[...] = x1
    xf = x1.astype(F32)
    ms = jnp.mean(xf * xf, axis=1, keepdims=True)
    h2 = (xf * lax.rsqrt(ms + NORM_EPS) * lnm_ref[...].astype(F32)[None, :]).astype(BF16)
    h2_ref[...] = h2
    logits = lax.dot_general(wr_ref[...], h2, (((1,), (1,)), ((), ())), preferred_element_type=F32)
    top_k = topk_ref.shape[0]
    n_exp = wr_ref.shape[0]
    n_dev = ri_ref.shape[1]
    e_local = n_exp // n_dev
    exp_id = lax.broadcasted_iota(jnp.int32, (n_exp, n_tok), 0)
    picked = [jnp.sum(jnp.where(exp_id == topk_ref[pl.ds(k, 1), :], logits, 0.0), axis=0, keepdims=True) for k in range(top_k)]
    picked = jnp.concatenate(picked, axis=0)
    ex = jnp.exp(picked - jnp.max(picked, axis=0, keepdims=True))
    gate = ex / jnp.sum(ex, axis=0, keepdims=True)
    dev_id = lax.broadcasted_iota(jnp.int32, (n_dev, n_tok), 0)
    r_dev = jnp.zeros((n_dev, n_tok), F32)
    i_dev = jnp.zeros((n_dev, n_tok), F32)
    for k in range(top_k):
        idx = topk_ref[pl.ds(k, 1), :]
        dev = idx // e_local
        mine = dev_id == dev
        r_dev = r_dev + jnp.where(mine, gate[k:k + 1], 0.0)
        i_dev = i_dev + jnp.where(mine, (idx - dev * e_local).astype(F32), 0.0)
    ri_ref[0] = r_dev
    ri_ref[1] = i_dev

    def drain(g, carry):
        for c in writes(g):
            c.wait()
        return carry

    lax.fori_loop(0, n_head, drain, 0)


def attn_kernel(n_small, *refs):
    small, rest = refs[:n_small], refs[n_small:]
    held, sem = rest[-n_small - 1:-1], rest[-1]
    copies = [pltpu.make_async_copy(src, dst, sem.at[i]) for i, (src, dst) in enumerate(zip(small, held))]
    attn_body(copies, *held, *rest[:-n_small - 1])


def in_hbm(arrays):
    return [pltpu.with_memory_space_constraint(a, pltpu.HBM) for a in arrays]


def attention(x_in, k_cache, v_cache, cache_len, topk_idx, ln_attn, w_q, w_k, w_v, q_norm, k_norm, w_o, ln_moe, w_router, ep_size):
    n_tok, hidden = x_in.shape
    _, n_slots, kv_heads, head_dim = k_cache.shape
    freq = np.float32(ROPE_BASE) ** (-np.arange(head_dim // 2, dtype=np.float32) * np.float32(2.0) / np.float32(head_dim))
    freq = jnp.asarray(np.ascontiguousarray(np.broadcast_to(freq[:, None], (head_dim // 2, 128))), F32)
    kt = k_cache.transpose(1, 2, 3, 0)
    vt = v_cache.transpose(1, 2, 3, 0)
    vmem = pl.BlockSpec(memory_space=pltpu.VMEM)
    hbm = pl.BlockSpec(memory_space=pltpu.HBM)
    dma = pltpu.SemaphoreType.DMA
    small = [freq, x_in, cache_len.reshape(1, n_tok), topk_idx.T, ln_attn, q_norm.reshape(1, head_dim), k_norm.reshape(1, head_dim), ln_moe, w_router.T]
    out = pl.pallas_call(
        functools.partial(attn_kernel, len(small)),
        in_specs=[hbm] * (len(small) + 6),
        out_specs=[vmem, vmem, vmem, hbm, hbm],
        out_shape=[
            jax.ShapeDtypeStruct((n_tok, hidden), BF16), jax.ShapeDtypeStruct((n_tok, hidden), BF16), jax.ShapeDtypeStruct((2, ep_size, n_tok), F32),
            jax.ShapeDtypeStruct(kt.shape, BF16), jax.ShapeDtypeStruct(vt.shape, BF16),
        ],
        scratch_shapes=[
            pltpu.VMEM(w_q.shape, BF16), pltpu.VMEM(w_k.shape, BF16), pltpu.VMEM(w_v.shape, BF16), pltpu.VMEM(w_o.shape, BF16),
            pltpu.VMEM((kv_heads, n_slots, head_dim, n_tok), BF16), pltpu.VMEM((kv_heads, n_slots, head_dim, n_tok), BF16),
            pltpu.VMEM((n_tok, hidden), BF16), pltpu.VMEM((head_dim // 2, n_tok), F32), pltpu.VMEM((head_dim // 2, n_tok), F32),
            pltpu.VMEM((head_dim, 128), F32), pltpu.VMEM((head_dim, 128), F32), pltpu.VMEM((16, n_tok), BF16),
            pltpu.VMEM((2 * kv_heads, head_dim, n_tok), F32), pltpu.VMEM((kv_heads, head_dim, n_tok), BF16), pltpu.VMEM((kv_heads, head_dim, n_tok), BF16),
            pltpu.VMEM((2, n_slots, n_tok), F32), pltpu.VMEM((n_tok, w_q.shape[1]), BF16),
            dma((4,)), dma((kv_heads,)), dma((kv_heads,)), dma((kv_heads,)), dma((kv_heads,)),
        ] + [pltpu.VMEM(a.shape, a.dtype) for a in small] + [dma((len(small),))],
        compiler_params=pltpu.CompilerParams(vmem_limit_bytes=40 << 20),
        name="attend",
    )(*in_hbm(small + [w_q, w_k, w_v, w_o, kt, vt]))
    x1, h2, ri, kto, vto = out
    return x1, h2, ri, kto.transpose(3, 0, 1, 2), vto.transpose(3, 0, 1, 2)


def moe_kernel(n_chip, h2_ref, ri_ref, x1_ref, wg_hbm, wu_hbm, wd_hbm, out_ref,
               wg, wu, wd, hbuf, gsrc, gbuf, xm, gm, m_scr, ybuf, y_near, y_far, y_peer, y_own, s_out, s_in, acc_scr,
               w_sem, send_h, recv_h, send_p, recv_p, send_g, recv_g, send_n, recv_n, send_f, recv_f, send_y, recv_y, send_s, recv_s):
    ep = lax.axis_index("ep")
    core = lax.rem(ep, 2)
    chip = ep // 2
    right = lax.rem(chip + 1, n_chip)
    left = lax.rem(chip + n_chip - 1, n_chip)
    opp = lax.rem(chip + 2, n_chip)
    other = 1 - core
    n_tok, hidden = h2_ref.shape
    hb = n_tok // 2
    qb = hb // 2
    e_local = wg.shape[0] // hidden
    ff = wg.shape[1]

    def dev(ch, co):
        return {"ep": ch * 2 + co}

    def rcopy(src, dst, ssem, rsem, ch, co):
        return pltpu.make_async_remote_copy(src_ref=src, dst_ref=dst, send_sem=ssem, recv_sem=rsem, device_id=dev(ch, co), device_id_type=MESH)

    top = pl.ds(0, hb)
    bot = pl.ds(hb, hb)

    w_copies = [pltpu.make_async_copy(wg_hbm, wg, w_sem.at[0]), pltpu.make_async_copy(wu_hbm, wu, w_sem.at[1]), pltpu.make_async_copy(wd_hbm, wd, w_sem.at[2])]

    dispatch = {
        1: rcopy(h2_ref.at[top], hbuf.at[1, top], send_h.at[1], recv_h.at[1], right, core),
        2: rcopy(h2_ref.at[bot], hbuf.at[2, top], send_h.at[2], recv_h.at[2], left, core),
        5: rcopy(h2_ref.at[bot], hbuf.at[5, top], send_h.at[5], recv_h.at[5], right, core),
        6: rcopy(h2_ref.at[top], hbuf.at[6, top], send_h.at[6], recv_h.at[6], left, core),
        3: rcopy(hbuf.at[1, top], hbuf.at[3, top], send_h.at[3], recv_h.at[3], right, core),
        4: rcopy(hbuf.at[2, top], hbuf.at[4, top], send_h.at[4], recv_h.at[4], left, core),
    }
    to_peer = {u: rcopy(hbuf.at[u, top], hbuf.at[u, bot], send_p.at[u], recv_p.at[u], chip, other) for u in range(1, 7)}
    to_peer[7] = rcopy(h2_ref, hbuf.at[7], send_p.at[7], recv_p.at[7], chip, other)
    gate = {}
    for rel, ch in ((0, chip), (1, right), (2, opp), (3, left)):
        for q, co in ((0, core), (1, other)):
            if rel or q:
                gate[2 * rel + q] = rcopy(ri_ref, gsrc.at[2 * rel + q], send_g.at[2 * rel + q], recv_g.at[2 * rel + q], ch, co)

    near = {}
    far = {}
    for u, ch, slot in ((1, left, 0), (2, right, 1)):
        near[u] = [rcopy(ybuf.at[u, top], y_near.at[slot, core], send_n.at[slot, 0], recv_n.at[slot, core], ch, core),
                   rcopy(ybuf.at[u, bot], y_near.at[slot, core], send_n.at[slot, 1], recv_n.at[slot, core], ch, other)]
    for u, ch, slot in ((3, right, 1), (4, left, 0)):
        far[u] = []
        for p in range(2):
            rows = pl.ds(p * qb, qb)
            far[u].append(rcopy(ybuf.at[u, rows], y_far.at[slot, core, rows], send_f.at[slot, p, 0], recv_f.at[slot, core, p], ch, core))
            far[u].append(rcopy(ybuf.at[u, pl.ds(hb + p * qb, qb)], y_far.at[slot, core, rows], send_f.at[slot, p, 1], recv_f.at[slot, core, p], ch, other))
    peer_y = {5: rcopy(ybuf.at[5, bot], y_peer.at[0], send_y.at[0], recv_y.at[0], chip, other),
              6: rcopy(ybuf.at[6, bot], y_peer.at[1], send_y.at[1], recv_y.at[1], chip, other),
              7: rcopy(ybuf.at[7], y_own, send_y.at[2], recv_y.at[2], chip, other)}
    sums = {}
    for p in range(2):
        rows = pl.ds(p * qb, qb)
        sums[0, p] = rcopy(s_out.at[0, rows], s_in.at[1, rows], send_s.at[0, p], recv_s.at[1, p], left, core)
        sums[1, p] = rcopy(s_out.at[1, rows], s_in.at[0, rows], send_s.at[1, p], recv_s.at[0, p], right, core)

    barrier = pltpu.get_barrier_semaphore()
    for d in range(1, 2 * n_chip):
        pl.semaphore_signal(barrier, inc=1, device_id={"ep": lax.rem(ep + d, 2 * n_chip)}, device_id_type=MESH)
    for c in w_copies:
        c.start()
    pl.semaphore_wait(barrier, 2 * n_chip - 1)

    dispatch[1].start()
    dispatch[2].start()
    for c in gate.values():
        c.start()
    dispatch[5].start()
    dispatch[6].start()
    to_peer[7].start()
    hbuf[0] = h2_ref[...]
    gbuf[0] = ri_ref[...]

    dev_iota = lax.broadcasted_iota(jnp.int32, (2 * n_chip, 128), 0)

    def row_of(block, d):
        return jnp.sum(jnp.where(dev_iota == d, block, 0.0), axis=0, keepdims=True)

    def columns(rows):
        rows = rows + [jnp.zeros((128 - len(rows), 128), F32)]
        return jnp.concatenate(rows, axis=0).T

    def compute(u, count):
        n_rows = count * n_tok
        for hf in range(2 * count):
            v = u + hf // 2
            src = pl.ds((hf % 2) * hb, hb)
            rs = pl.ds(hf * hb, hb)
            ids = row_of(gbuf[v, 1, :, src], ep)
            cols = columns([(ids == float(e)).astype(F32) for e in range(e_local)])
            for e in range(e_local):
                keep = jnp.broadcast_to(cols[:, e:e + 1], (hb, 128)).astype(BF16)
                m_scr[e, rs, :] = keep
                for b in range(hidden // 128):
                    xm[rs, e * hidden + b * 128:e * hidden + (b + 1) * 128] = hbuf[v, src, b * 128:(b + 1) * 128] * keep
        rows = pl.ds(0, n_rows)

        def up_tile(n, carry):
            cs = pl.ds(pl.multiple_of(n * 256, 256), 256)
            a = jnp.dot(xm[rows], wg[:, cs], preferred_element_type=F32)
            b = jnp.dot(xm[rows], wu[:, cs], preferred_element_type=F32)
            g = (a * (1.0 / (1.0 + jnp.exp(-a))) * b).astype(BF16)
            for e in range(e_local):
                for q in range(2):
                    gm[rows, pl.ds(pl.multiple_of(n * 256, 256) + e * ff + q * 128, 128)] = g[:, q * 128:(q + 1) * 128] * m_scr[e, rows]
            return carry

        lax.fori_loop(0, ff // 256, up_tile, 0)

        def down_tile(n, carry):
            cs = pl.ds(pl.multiple_of(n * 256, 256), 256)
            y = jnp.dot(gm[rows], wd[:, cs], preferred_element_type=F32).astype(BF16)
            for i in range(count):
                ybuf[u + i, :, cs] = y[i * n_tok:(i + 1) * n_tok]
            return carry

        lax.fori_loop(0, hidden // 256, down_tile, 0)

    def gate_cols(u, lanes, devs):
        blk = gbuf[u, 0, :, lanes]
        return columns([row_of(blk, d) for d in devs])

    def take_gate(u):
        if u == 7:
            gate[1].wait_recv()
            gbuf[7] = gsrc[1]
            return
        rel, hf = ((1, 0), (3, 1), (2, 0), (2, 1), (1, 1), (3, 0))[u - 1]
        for q in range(2):
            if u in (1, 2, 3):
                gate[2 * rel + q].wait_recv()
            gbuf[u, :, :, pl.ds(q * hb, hb)] = gsrc[2 * rel + q, :, :, pl.ds(hf * hb, hb)]

    def send_sums():
        for slot, u in ((0, 5), (1, 6)):
            peer_y[u].wait_recv()
        for p in range(2):
            rows = pl.ds(p * qb, qb)
            for slot, u, ch in ((0, 5, right), (1, 6, left)):
                for co in range(2):
                    piece = y_far.at[slot, co, rows]
                    rcopy(piece, piece, send_f.at[slot, p, co], recv_f.at[slot, co, p], ch, core).wait_recv()
                cols = gate_cols(u, pl.ds(0, 128), [ep, chip * 2 + other, ch * 2, ch * 2 + 1])[p * qb:(p + 1) * qb]
                s_out[slot, rows] = (ybuf[u, rows, :].astype(F32) * cols[:, 0:1] + y_peer[slot, rows].astype(F32) * cols[:, 1:2]
                                     + y_far[slot, 0, rows].astype(F32) * cols[:, 2:3] + y_far[slot, 1, rows].astype(F32) * cols[:, 3:4])
                sums[slot, p].start()

    def before(u):
        if u == 0:
            for c in w_copies:
                c.wait()
        if u == 1:
            for v in (1, 2):
                dispatch[v].wait_recv()
                dispatch[v + 2].start()
                to_peer[v].start()
        if u == 3:
            for v in (5, 6, 3, 4):
                dispatch[v].wait_recv()
                to_peer[v].start()
        if u == 7:
            send_sums()
        if u >= 1:
            to_peer[u].wait_recv()
            take_gate(u)

    def after(u):
        if u in (1, 2):
            for c in near[u]:
                c.start()
        if u in (3, 4):
            for c in far[u]:
                c.start()
        if u in (5, 6, 7):
            peer_y[u].start()

    rounds = ((0,), (1, 2), (3, 4), (5, 6), (7,))

    def unit_round(r, carry):
        for v, units in enumerate(rounds):
            @pl.when(r == v)
            def _():
                for u in units:
                    before(u)

        @pl.when(lax.rem(r, 4) == 0)
        def _():
            compute((r // 4) * 7, 1)

        @pl.when(lax.rem(r, 4) != 0)
        def _():
            compute(2 * r - 1, 2)

        for v, units in enumerate(rounds):
            @pl.when(r == v)
            def _():
                for u in units:
                    after(u)
        return carry

    lax.fori_loop(0, len(rounds), unit_round, 0)

    peer_y[7].wait_recv()
    for hf, ch in ((0, right), (1, left)):
        rs = pl.ds(hf * hb, hb)
        for co in range(2):
            rcopy(y_near.at[hf, co], y_near.at[hf, co], send_n.at[hf, co], recv_n.at[hf, co], ch, core).wait_recv()
        cols = gate_cols(0, rs, [ep, chip * 2 + other, ch * 2, ch * 2 + 1])
        acc_scr[rs, :] = x1_ref[rs, :].astype(F32) + (
            ybuf[0, rs, :].astype(F32) * cols[:, 0:1] + y_own[rs, :].astype(F32) * cols[:, 1:2]
            + y_near[hf, 0].astype(F32) * cols[:, 2:3] + y_near[hf, 1].astype(F32) * cols[:, 3:4])
    for p in range(2):
        for hf in range(2):
            rows = pl.ds(p * qb, qb)
            rs = pl.ds(hf * hb + p * qb, qb)
            sums[1 - hf, p].wait_recv()
            out_ref[rs, :] = (acc_scr[rs, :] + s_in[hf, rows]).astype(BF16)

    for group in (list(dispatch.values()), list(gate.values()), list(to_peer.values()), near[1], near[2], far[3], far[4], list(peer_y.values()), list(sums.values())):
        for c in group:
            c.wait_send()


def moe(h2, ri, x1, w_gate, w_up, w_down, ep_size):
    n_tok, hidden = h2.shape
    e_local, _, ff = w_gate.shape
    hb = n_tok // 2
    dma = pltpu.SemaphoreType.DMA
    vmem = pl.BlockSpec(memory_space=pltpu.VMEM)
    hbm = pl.BlockSpec(memory_space=pltpu.HBM)
    return pl.pallas_call(
        functools.partial(moe_kernel, ep_size // 2),
        out_shape=jax.ShapeDtypeStruct((n_tok, hidden), BF16),
        in_specs=[vmem] * 3 + [hbm] * 3,
        out_specs=vmem,
        scratch_shapes=[
            pltpu.VMEM((e_local * hidden, ff), BF16), pltpu.VMEM((e_local * hidden, ff), BF16), pltpu.VMEM((e_local * ff, hidden), BF16),
            pltpu.VMEM((8, n_tok, hidden), BF16), pltpu.VMEM((8, 2, ep_size, n_tok), F32), pltpu.VMEM((8, 2, ep_size, n_tok), F32),
            pltpu.VMEM((2 * n_tok, e_local * hidden), BF16), pltpu.VMEM((2 * n_tok, e_local * ff), BF16), pltpu.VMEM((e_local, 2 * n_tok, 128), BF16),
            pltpu.VMEM((8, n_tok, hidden), BF16), pltpu.VMEM((2, 2, hb, hidden), BF16), pltpu.VMEM((2, 2, hb, hidden), BF16), pltpu.VMEM((2, hb, hidden), BF16), pltpu.VMEM((n_tok, hidden), BF16),
            pltpu.VMEM((2, hb, hidden), F32), pltpu.VMEM((2, hb, hidden), F32), pltpu.VMEM((n_tok, hidden), F32),
            dma((3,)), dma((8,)), dma((8,)), dma((8,)), dma((8,)), dma((8,)), dma((8,)), dma((2, 2)), dma((2, 2)), dma((2, 2, 2)), dma((2, 2, 2)), dma((3,)), dma((3,)), dma((2, 2)), dma((2, 2)),
        ],
        compiler_params=pltpu.CompilerParams(collective_id=0, has_side_effects=True, vmem_limit_bytes=46 << 20),
        name="moe",
    )(h2, ri, x1, *in_hbm([w_gate.reshape(e_local * hidden, ff), w_up.reshape(e_local * hidden, ff), w_down.reshape(e_local * ff, hidden)]))


def solution(mesh):
    ep_size = mesh.shape['ep']
    row_spec = P(('dp', 'ep'))
    replicated = P()
    expert_spec = P('ep')
    in_specs = (row_spec,) * 5 + (replicated,) * 9 + (expert_spec,) * 3

    def device_step(x_in, k_cache, v_cache, cache_len, topk_idx, ln_attn, w_q, w_k, w_v, q_norm, k_norm, w_o, ln_moe, w_router, w_gate, w_up, w_down):
        x1, h2, ri, k_new, v_new = attention(x_in, k_cache, v_cache, cache_len, topk_idx, ln_attn, w_q, w_k, w_v, q_norm, k_norm, w_o, ln_moe, w_router, ep_size)
        return moe(h2, ri, x1, w_gate, w_up, w_down, ep_size), k_new, v_new

    return jax.shard_map(device_step, mesh=mesh, in_specs=in_specs, out_specs=(row_spec,) * 3, check_vma=False)
```

```python
import functools

import jax
import jax.numpy as jnp
import numpy as np
from jax import lax
from jax.experimental import pallas as pl
from jax.experimental.pallas import tpu as pltpu
from jax.sharding import PartitionSpec as P

ROPE_BASE = 1000000.0
NORM_EPS = 1e-6
F32 = jnp.float32
BF16 = jnp.bfloat16
MESH = pl.DeviceIdType.MESH


def sublane_sums(parts):
    row = lax.broadcasted_iota(jnp.int32, parts[0].shape, 0)
    for d in (1, 2, 4):
        low = (row & d) == 0
        parts = [jnp.where(low, a, b) + pltpu.roll(jnp.where(low, b, a), d, 0) for a, b in zip(parts[0::2], parts[1::2])]
    return parts[0]


def attn_body(small_copies, freq_ref, x_ref, len_ref, topk_ref, lna_ref, qn_ref, kn_ref, lnm_ref, wr_ref, wq_hbm, wk_hbm, wv_hbm, wo_hbm, kc_hbm, vc_hbm,
                x1_ref, h2_ref, ri_ref, kco_hbm, vco_hbm,
                wq_scr, wk_scr, wv_scr, wo_scr, kbuf, vbuf, h_scr, cos_scr, sin_scr, qg_scr, kg_scr, len_scr, q_scr, kn_scr, vn_scr, s_scr, o_scr,
                w_sem, kin_sem, vin_sem, kout_sem, vout_sem):
    n_tok = x_ref.shape[0]
    n_head, n_slots, head_dim, _ = kbuf.shape
    half = head_dim // 2
    n_lt = n_tok // 128
    early = 1
    ahead = 4

    w_copies = [pltpu.make_async_copy(src, dst, w_sem.at[i]) for i, (src, dst) in enumerate(((wk_hbm, wk_scr), (wv_hbm, wv_scr), (wq_hbm, wq_scr), (wo_hbm, wo_scr)))]

    def reads(g):
        return (pltpu.make_async_copy(kc_hbm.at[:, g], kbuf.at[g], kin_sem.at[g]), pltpu.make_async_copy(vc_hbm.at[:, g], vbuf.at[g], vin_sem.at[g]))

    def writes(g):
        return (pltpu.make_async_copy(kbuf.at[g], kco_hbm.at[:, g], kout_sem.at[g]), pltpu.make_async_copy(vbuf.at[g], vco_hbm.at[:, g], vout_sem.at[g]))

    for c in small_copies + w_copies[:3]:
        c.start()
    for g in range(early):
        for c in reads(g):
            c.start()
    for c in small_copies:
        c.wait()

    xf = x_ref[...].astype(F32)
    ms = jnp.mean(xf * xf, axis=1, keepdims=True)
    h_scr[...] = (xf * lax.rsqrt(ms + NORM_EPS) * lna_ref[...].astype(F32)[None, :]).astype(BF16)
    lens = len_ref[...].astype(F32)
    angles = jnp.concatenate([freq_ref[...]] * n_lt, axis=1) * lens
    cos_scr[...] = jnp.cos(angles)
    sin_scr[...] = jnp.sin(angles)
    for src, dst in ((qn_ref, qg_scr), (kn_ref, kg_scr)):
        row = src[...].astype(F32)
        dst[...] = jnp.broadcast_to(jnp.concatenate([row, row], axis=1), (128, 128)).T[:head_dim]
    len_scr[...] = jnp.broadcast_to(lens, (16, n_tok)).astype(BF16)

    def head_rope(block, gain_scr):
        ms = jnp.mean(block * block, axis=0, keepdims=True)
        gain = jnp.concatenate([gain_scr[...]] * n_lt, axis=1)
        block = block * lax.rsqrt(ms + NORM_EPS) * gain
        lo, hi = block[:half], block[half:]
        cosv, sinv = cos_scr[...], sin_scr[...]
        return jnp.concatenate([lo * cosv - hi * sinv, hi * cosv + lo * sinv], axis=0).astype(BF16)

    per = 256 // head_dim
    for c in w_copies[:3]:
        c.wait()
    for g in range(early, ahead):
        for c in reads(g):
            c.start()
    w_copies[3].start()

    def project(w_scr, i):
        cols = pl.ds(pl.multiple_of(i * 256, 256), 256)
        return jnp.dot(h_scr[...], w_scr[:, cols], preferred_element_type=F32).T

    def kv_proj(i, carry):
        k_t = project(wk_scr, i)
        v_t = project(wv_scr, i)
        for j in range(per):
            kn_scr[i * per + j] = head_rope(k_t[j * head_dim:(j + 1) * head_dim], kg_scr)
            vn_scr[i * per + j] = v_t[j * head_dim:(j + 1) * head_dim].astype(BF16)
        return carry

    def q_proj(i, carry):
        q_t = project(wq_scr, i)
        for j in range(per):
            q_scr[i * per + j] = head_rope(q_t[j * head_dim:(j + 1) * head_dim], qg_scr).astype(F32)
        return carry

    lax.fori_loop(0, n_head // per, kv_proj, 0, unroll=True)
    lax.fori_loop(0, 2 * n_head // per, q_proj, 0, unroll=True)

    tiles = [pl.ds(r * 16, 16) for r in range(head_dim // 16)]

    def head(g, carry):
        @pl.when(g + ahead < n_head)
        def _():
            for c in reads(g + ahead):
                c.start()

        for c in reads(g):
            c.wait()

        for lt in range(n_lt):
            lanes = pl.ds(lt * 128, 128)

            def score_block(i, carry):
                parts = [[], []]
                for si in range(8):
                    s = i * 8 + si
                    hit = len_scr[:, lanes] == s.astype(F32).astype(BF16)
                    accs = [None, None]
                    for t in tiles:
                        kb = kbuf[g, s, t, lanes]
                        kbuf[g, s, t, lanes] = jnp.where(hit, kn_scr[g, t, lanes], kb)
                        kf = kb.astype(F32)
                        for j in range(2):
                            prod = kf * q_scr[2 * g + j, t, lanes]
                            accs[j] = prod if accs[j] is None else accs[j] + prod
                    for j in range(2):
                        parts[j].append(accs[j][:8] + accs[j][8:])
                for j in range(2):
                    s_scr[j, pl.ds(pl.multiple_of(i * 8, 8), 8), lanes] = sublane_sums(parts[j])
                return carry

            lax.fori_loop(0, n_slots // 8, score_block, 0, unroll=2)
            slot = lax.broadcasted_iota(jnp.int32, (n_slots, 128), 0)
            len_row = len_ref[:, lanes]
            kn = kn_scr[g, :, lanes].astype(F32)
            vn = vn_scr[g, :, lanes].astype(F32)
            accs = []
            for j in range(2):
                fresh = jnp.sum(kn * q_scr[2 * g + j, :, lanes], axis=0, keepdims=True)
                sc = jnp.where(slot == len_row, fresh, s_scr[j, :, lanes]) * (head_dim ** -0.5)
                sc = jnp.where(slot <= len_row, sc, -1e30)
                ex = jnp.exp(sc - jnp.max(sc, axis=0, keepdims=True))
                pr = (ex / jnp.sum(ex, axis=0, keepdims=True)).astype(BF16).astype(F32)
                accs.append(jnp.sum(jnp.where(slot == len_row, pr, 0.0), axis=0, keepdims=True) * vn)
                s_scr[j, :, lanes] = jnp.where(slot == len_row, 0.0, pr)

            def value_block(i, accs):
                accs = [[a[r * 16:(r + 1) * 16] for r in range(len(tiles))] for a in accs]
                prob = [s_scr[j, pl.ds(pl.multiple_of(i * 8, 8), 8), lanes] for j in range(2)]
                for si in range(8):
                    s = i * 8 + si
                    hit = len_scr[:, lanes] == s.astype(F32).astype(BF16)
                    for r, t in enumerate(tiles):
                        vb = vbuf[g, s, t, lanes]
                        vbuf[g, s, t, lanes] = jnp.where(hit, vn_scr[g, t, lanes], vb)
                        vf = vb.astype(F32)
                        for j in range(2):
                            accs[j][r] = accs[j][r] + prob[j][si:si + 1] * vf
                return tuple(jnp.concatenate(a, axis=0) for a in accs)

            accs = lax.fori_loop(0, n_slots // 8, value_block, tuple(accs), unroll=2)
            o_scr[pl.ds(lt * 128, 128), pl.ds(pl.multiple_of(g * 128, 128), 128)] = jnp.concatenate(accs, axis=0).T.astype(BF16)
        for c in writes(g):
            c.start()
        return carry

    lax.fori_loop(0, n_head, head, 0)

    w_copies[3].wait()
    x1 = (x_ref[...].astype(F32) + jnp.dot(o_scr[...], wo_scr[...], preferred_element_type=F32)).astype(BF16)
    x1_ref[...] = x1
    xf = x1.astype(F32)
    ms = jnp.mean(xf * xf, axis=1, keepdims=True)
    h2 = (xf * lax.rsqrt(ms + NORM_EPS) * lnm_ref[...].astype(F32)[None, :]).astype(BF16)
    h2_ref[...] = h2
    logits = lax.dot_general(wr_ref[...], h2, (((1,), (1,)), ((), ())), preferred_element_type=F32)
    top_k = topk_ref.shape[0]
    n_exp = wr_ref.shape[0]
    n_dev = ri_ref.shape[1]
    e_local = n_exp // n_dev
    exp_id = lax.broadcasted_iota(jnp.int32, (n_exp, n_tok), 0)
    picked = [jnp.sum(jnp.where(exp_id == topk_ref[pl.ds(k, 1), :], logits, 0.0), axis=0, keepdims=True) for k in range(top_k)]
    picked = jnp.concatenate(picked, axis=0)
    ex = jnp.exp(picked - jnp.max(picked, axis=0, keepdims=True))
    gate = ex / jnp.sum(ex, axis=0, keepdims=True)
    dev_id = lax.broadcasted_iota(jnp.int32, (n_dev, n_tok), 0)
    r_dev = jnp.zeros((n_dev, n_tok), F32)
    i_dev = jnp.zeros((n_dev, n_tok), F32)
    for k in range(top_k):
        idx = topk_ref[pl.ds(k, 1), :]
        dev = idx // e_local
        mine = dev_id == dev
        r_dev = r_dev + jnp.where(mine, gate[k:k + 1], 0.0)
        i_dev = i_dev + jnp.where(mine, (idx - dev * e_local).astype(F32), 0.0)
    ri_ref[0] = r_dev
    ri_ref[1] = i_dev

    def drain(g, carry):
        for c in writes(g):
            c.wait()
        return carry

    lax.fori_loop(0, n_head, drain, 0)


def attn_kernel(n_small, *refs):
    small, rest = refs[:n_small], refs[n_small:]
    held, sem = rest[-n_small - 1:-1], rest[-1]
    copies = [pltpu.make_async_copy(src, dst, sem.at[i]) for i, (src, dst) in enumerate(zip(small, held))]
    attn_body(copies, *held, *rest[:-n_small - 1])


def in_hbm(arrays):
    return [pltpu.with_memory_space_constraint(a, pltpu.HBM) for a in arrays]


def attention(x_in, k_cache, v_cache, cache_len, topk_idx, ln_attn, w_q, w_k, w_v, q_norm, k_norm, w_o, ln_moe, w_router, ep_size):
    n_tok, hidden = x_in.shape
    _, n_slots, kv_heads, head_dim = k_cache.shape
    freq = np.float32(ROPE_BASE) ** (-np.arange(head_dim // 2, dtype=np.float32) * np.float32(2.0) / np.float32(head_dim))
    freq = jnp.asarray(np.ascontiguousarray(np.broadcast_to(freq[:, None], (head_dim // 2, 128))), F32)
    kt = k_cache.transpose(1, 2, 3, 0)
    vt = v_cache.transpose(1, 2, 3, 0)
    vmem = pl.BlockSpec(memory_space=pltpu.VMEM)
    hbm = pl.BlockSpec(memory_space=pltpu.HBM)
    dma = pltpu.SemaphoreType.DMA
    small = [freq, x_in, cache_len.reshape(1, n_tok), topk_idx.T, ln_attn, q_norm.reshape(1, head_dim), k_norm.reshape(1, head_dim), ln_moe, w_router.T]
    out = pl.pallas_call(
        functools.partial(attn_kernel, len(small)),
        in_specs=[hbm] * (len(small) + 6),
        out_specs=[vmem, vmem, vmem, hbm, hbm],
        out_shape=[
            jax.ShapeDtypeStruct((n_tok, hidden), BF16), jax.ShapeDtypeStruct((n_tok, hidden), BF16), jax.ShapeDtypeStruct((2, ep_size, n_tok), F32),
            jax.ShapeDtypeStruct(kt.shape, BF16), jax.ShapeDtypeStruct(vt.shape, BF16),
        ],
        scratch_shapes=[
            pltpu.VMEM(w_q.shape, BF16), pltpu.VMEM(w_k.shape, BF16), pltpu.VMEM(w_v.shape, BF16), pltpu.VMEM(w_o.shape, BF16),
            pltpu.VMEM((kv_heads, n_slots, head_dim, n_tok), BF16), pltpu.VMEM((kv_heads, n_slots, head_dim, n_tok), BF16),
            pltpu.VMEM((n_tok, hidden), BF16), pltpu.VMEM((head_dim // 2, n_tok), F32), pltpu.VMEM((head_dim // 2, n_tok), F32),
            pltpu.VMEM((head_dim, 128), F32), pltpu.VMEM((head_dim, 128), F32), pltpu.VMEM((16, n_tok), BF16),
            pltpu.VMEM((2 * kv_heads, head_dim, n_tok), F32), pltpu.VMEM((kv_heads, head_dim, n_tok), BF16), pltpu.VMEM((kv_heads, head_dim, n_tok), BF16),
            pltpu.VMEM((2, n_slots, n_tok), F32), pltpu.VMEM((n_tok, w_q.shape[1]), BF16),
            dma((4,)), dma((kv_heads,)), dma((kv_heads,)), dma((kv_heads,)), dma((kv_heads,)),
        ] + [pltpu.VMEM(a.shape, a.dtype) for a in small] + [dma((len(small),))],
        compiler_params=pltpu.CompilerParams(vmem_limit_bytes=40 << 20),
        name="attend",
    )(*in_hbm(small + [w_q, w_k, w_v, w_o, kt, vt]))
    x1, h2, ri, kto, vto = out
    return x1, h2, ri, kto.transpose(3, 0, 1, 2), vto.transpose(3, 0, 1, 2)


def moe_kernel(n_chip, h2_ref, ri_ref, x1_ref, wg_hbm, wu_hbm, wd_hbm, out_ref,
               wg, wu, wd, hbuf, gsrc, gbuf, xm, gm, m_scr, ybuf, y_near, y_far, y_peer, y_own, s_out, s_in, acc_scr,
               w_sem, send_h, recv_h, send_p, recv_p, send_g, recv_g, send_n, recv_n, send_f, recv_f, send_y, recv_y, send_s, recv_s):
    ep = lax.axis_index("ep")
    core = lax.rem(ep, 2)
    chip = ep // 2
    right = lax.rem(chip + 1, n_chip)
    left = lax.rem(chip + n_chip - 1, n_chip)
    opp = lax.rem(chip + 2, n_chip)
    other = 1 - core
    n_tok, hidden = h2_ref.shape
    hb = n_tok // 2
    qb = hb // 2
    e_local = wg.shape[0] // hidden
    ff = wg.shape[1]

    def dev(ch, co):
        return {"ep": ch * 2 + co}

    def rcopy(src, dst, ssem, rsem, ch, co):
        return pltpu.make_async_remote_copy(src_ref=src, dst_ref=dst, send_sem=ssem, recv_sem=rsem, device_id=dev(ch, co), device_id_type=MESH)

    top = pl.ds(0, hb)
    bot = pl.ds(hb, hb)

    w_copies = [pltpu.make_async_copy(src, dst, w_sem.at[i]) for i, (src, dst) in enumerate(((wg_hbm, wg), (wu_hbm, wu), (wd_hbm, wd)))]

    q0 = pl.ds(0, qb)
    q1 = pl.ds(qb, qb)
    dispatch = {}
    for key, u, src, rows, ch in (
        (1, 1, h2_ref.at[top], top, right), (2, 2, h2_ref.at[bot], top, left), (3, 3, hbuf.at[1, top], top, right), (4, 4, hbuf.at[2, top], top, left),
        (5, 5, h2_ref.at[pl.ds(hb, qb)], q0, right), (6, 6, h2_ref.at[q0], q0, left), (0, 5, h2_ref.at[pl.ds(hb + qb, qb)], q1, right), (7, 6, h2_ref.at[q1], q1, left),
    ):
        dispatch[key] = rcopy(src, hbuf.at[u, rows], send_h.at[key], recv_h.at[key], ch, core)
    to_peer = {u: rcopy(hbuf.at[u, top], hbuf.at[u, bot], send_p.at[u], recv_p.at[u], chip, other) for u in range(1, 7)}
    to_peer[7] = rcopy(h2_ref, hbuf.at[7], send_p.at[7], recv_p.at[7], chip, other)
    gate = {}
    for rel, ch in ((0, chip), (1, right), (2, opp), (3, left)):
        for q, co in ((0, core), (1, other)):
            if rel or q:
                gate[2 * rel + q] = rcopy(ri_ref, gsrc.at[2 * rel + q], send_g.at[2 * rel + q], recv_g.at[2 * rel + q], ch, co)

    near = {}
    far = {}
    for u, ch, slot in ((1, left, 0), (2, right, 1)):
        near[u] = [rcopy(ybuf.at[u, top], y_near.at[slot, core], send_n.at[slot, 0], recv_n.at[slot, core], ch, core),
                   rcopy(ybuf.at[u, bot], y_near.at[slot, core], send_n.at[slot, 1], recv_n.at[slot, core], ch, other)]
    for u, ch, slot in ((3, right, 1), (4, left, 0)):
        far[u] = []
        for p in range(2):
            rows = pl.ds(p * qb, qb)
            far[u].append(rcopy(ybuf.at[u, rows], y_far.at[slot, core, rows], send_f.at[slot, p, 0], recv_f.at[slot, core, p], ch, core))
            far[u].append(rcopy(ybuf.at[u, pl.ds(hb + p * qb, qb)], y_far.at[slot, core, rows], send_f.at[slot, p, 1], recv_f.at[slot, core, p], ch, other))
    peer_y = {u: rcopy(ybuf.at[u, bot], y_peer.at[i], send_y.at[i], recv_y.at[i], chip, other) for i, u in enumerate((5, 6))}
    peer_y[7] = rcopy(ybuf.at[7], y_own, send_y.at[2], recv_y.at[2], chip, other)
    sums = {}
    for p in range(2):
        rows = pl.ds(p * qb, qb)
        sums[0, p] = rcopy(s_out.at[0, rows], s_in.at[1, rows], send_s.at[0, p], recv_s.at[1, p], left, core)
        sums[1, p] = rcopy(s_out.at[1, rows], s_in.at[0, rows], send_s.at[1, p], recv_s.at[0, p], right, core)

    barrier = pltpu.get_barrier_semaphore()
    for d in range(1, 2 * n_chip):
        pl.semaphore_signal(barrier, inc=1, device_id={"ep": lax.rem(ep + d, 2 * n_chip)}, device_id_type=MESH)
    for c in w_copies:
        c.start()
    pl.semaphore_wait(barrier, 2 * n_chip - 1)

    dispatch[1].start()
    dispatch[2].start()
    for c in gate.values():
        c.start()
    dispatch[5].start()
    dispatch[6].start()
    to_peer[7].start()
    hbuf[0] = h2_ref[...]
    gbuf[0] = ri_ref[...]

    dev_iota = lax.broadcasted_iota(jnp.int32, (2 * n_chip, 128), 0)

    def row_of(block, d):
        return jnp.sum(jnp.where(dev_iota == d, block, 0.0), axis=0, keepdims=True)

    def columns(rows):
        rows = rows + [jnp.zeros((128 - len(rows), 128), F32)]
        return jnp.concatenate(rows, axis=0).T

    def compute(u, count):
        n_rows = count * n_tok
        for hf in range(2 * count):
            v = u + hf // 2
            src = pl.ds((hf % 2) * hb, hb)
            rs = pl.ds(hf * hb, hb)
            ids = row_of(gbuf[v, 1, :, src], ep)
            cols = columns([(ids == float(e)).astype(F32) for e in range(e_local)])
            for e in range(e_local):
                keep = jnp.broadcast_to(cols[:, e:e + 1], (hb, 128)).astype(BF16)
                m_scr[e, rs, :] = keep
                for b in range(hidden // 128):
                    xm[rs, e * hidden + b * 128:e * hidden + (b + 1) * 128] = hbuf[v, src, b * 128:(b + 1) * 128] * keep
        rows = pl.ds(0, n_rows)

        def up_tile(n, carry):
            cs = pl.ds(pl.multiple_of(n * 256, 256), 256)
            a = jnp.dot(xm[rows], wg[:, cs], preferred_element_type=F32)
            b = jnp.dot(xm[rows], wu[:, cs], preferred_element_type=F32)
            g = (a * (1.0 / (1.0 + jnp.exp(-a))) * b).astype(BF16)
            for e in range(e_local):
                for q in range(2):
                    gm[rows, pl.ds(pl.multiple_of(n * 256, 256) + e * ff + q * 128, 128)] = g[:, q * 128:(q + 1) * 128] * m_scr[e, rows]
            return carry

        lax.fori_loop(0, ff // 256, up_tile, 0)

        def down_tile(n, carry):
            cs = pl.ds(pl.multiple_of(n * 256, 256), 256)
            y = jnp.dot(gm[rows], wd[:, cs], preferred_element_type=F32).astype(BF16)
            for i in range(count):
                ybuf[u + i, :, cs] = y[i * n_tok:(i + 1) * n_tok]
            return carry

        lax.fori_loop(0, hidden // 256, down_tile, 0)

    def gate_cols(u, lanes, devs):
        blk = gbuf[u, 0, :, lanes]
        cols = columns([row_of(blk, d) for d in devs])
        return [cols[:, i:i + 1] for i in range(len(devs))]

    def take_gate(u):
        if u == 7:
            gate[1].wait_recv()
            gbuf[7] = gsrc[1]
            return
        rel, hf = ((1, 0), (3, 1), (2, 0), (2, 1), (1, 1), (3, 0))[u - 1]
        for q in range(2):
            if u in (1, 2, 3):
                gate[2 * rel + q].wait_recv()
            gbuf[u, :, :, pl.ds(q * hb, hb)] = gsrc[2 * rel + q, :, :, pl.ds(hf * hb, hb)]

    def send_sums():
        for slot, u in ((0, 5), (1, 6)):
            peer_y[u].wait_recv()
        for p in range(2):
            rows = pl.ds(p * qb, qb)
            for slot, u, ch in ((0, 5, right), (1, 6, left)):
                for co in range(2):
                    piece = y_far.at[slot, co, rows]
                    rcopy(piece, piece, send_f.at[slot, p, co], recv_f.at[slot, co, p], ch, core).wait_recv()
                c_own, c_peer, c_a, c_b = [c[p * qb:(p + 1) * qb] for c in gate_cols(u, top, [ep, chip * 2 + other, ch * 2, ch * 2 + 1])]
                s_out[slot, rows] = (ybuf[u, rows, :].astype(F32) * c_own + y_peer[slot, rows].astype(F32) * c_peer
                                     + y_far[slot, 0, rows].astype(F32) * c_a + y_far[slot, 1, rows].astype(F32) * c_b)
                sums[slot, p].start()

    def before(u):
        if u == 0:
            for c in w_copies:
                c.wait()
        if u == 1:
            for v in (1, 2):
                dispatch[v].wait_recv()
                dispatch[v + 2].start()
                to_peer[v].start()
            dispatch[0].start()
            dispatch[7].start()
        if u == 3:
            for v in (3, 4):
                dispatch[v].wait_recv()
                to_peer[v].start()
        if u == 5:
            for v, w in ((5, 0), (6, 7)):
                dispatch[v].wait_recv()
                dispatch[w].wait_recv()
                to_peer[v].start()
        if u == 7:
            send_sums()
        if u >= 1:
            to_peer[u].wait_recv()
            take_gate(u)

    def after(u):
        if u in (1, 2):
            for c in near[u]:
                c.start()
        if u in (3, 4):
            for c in far[u]:
                c.start()
        if u in (5, 6, 7):
            peer_y[u].start()

    rounds = ((0,), (1, 2), (3, 4), (5, 6), (7,))

    def unit_round(r, carry):
        for v, units in enumerate(rounds):
            @pl.when(r == v)
            def _():
                for u in units:
                    before(u)

        @pl.when(lax.rem(r, 4) == 0)
        def _():
            compute((r // 4) * 7, 1)

        @pl.when(lax.rem(r, 4) != 0)
        def _():
            compute(2 * r - 1, 2)

        for v, units in enumerate(rounds):
            @pl.when(r == v)
            def _():
                for u in units:
                    after(u)
        return carry

    lax.fori_loop(0, len(rounds), unit_round, 0)

    peer_y[7].wait_recv()
    for hf, ch in ((0, right), (1, left)):
        rs = pl.ds(hf * hb, hb)
        for co in range(2):
            rcopy(y_near.at[hf, co], y_near.at[hf, co], send_n.at[hf, co], recv_n.at[hf, co], ch, core).wait_recv()
        c_own, c_peer, c_a, c_b = gate_cols(0, rs, [ep, chip * 2 + other, ch * 2, ch * 2 + 1])
        acc_scr[rs, :] = x1_ref[rs, :].astype(F32) + (
            ybuf[0, rs, :].astype(F32) * c_own + y_own[rs, :].astype(F32) * c_peer
            + y_near[hf, 0].astype(F32) * c_a + y_near[hf, 1].astype(F32) * c_b)
    for p in range(2):
        for hf in range(2):
            rows = pl.ds(p * qb, qb)
            rs = pl.ds(hf * hb + p * qb, qb)
            sums[1 - hf, p].wait_recv()
            out_ref[rs, :] = (acc_scr[rs, :] + s_in[hf, rows]).astype(BF16)

    for group in (list(dispatch.values()), list(gate.values()), list(to_peer.values()), near[1], near[2], far[3], far[4], list(peer_y.values()), list(sums.values())):
        for c in group:
            c.wait_send()


def moe(h2, ri, x1, w_gate, w_up, w_down, ep_size):
    n_tok, hidden = h2.shape
    e_local, _, ff = w_gate.shape
    hb = n_tok // 2
    dma = pltpu.SemaphoreType.DMA
    vmem = pl.BlockSpec(memory_space=pltpu.VMEM)
    hbm = pl.BlockSpec(memory_space=pltpu.HBM)
    return pl.pallas_call(
        functools.partial(moe_kernel, ep_size // 2),
        out_shape=jax.ShapeDtypeStruct((n_tok, hidden), BF16),
        in_specs=[vmem] * 3 + [hbm] * 3,
        out_specs=vmem,
        scratch_shapes=[
            pltpu.VMEM((e_local * hidden, ff), BF16), pltpu.VMEM((e_local * hidden, ff), BF16), pltpu.VMEM((e_local * ff, hidden), BF16),
            pltpu.VMEM((8, n_tok, hidden), BF16), pltpu.VMEM((8, 2, ep_size, n_tok), F32), pltpu.VMEM((8, 2, ep_size, n_tok), F32),
            pltpu.VMEM((2 * n_tok, e_local * hidden), BF16), pltpu.VMEM((2 * n_tok, e_local * ff), BF16), pltpu.VMEM((e_local, 2 * n_tok, 128), BF16),
            pltpu.VMEM((8, n_tok, hidden), BF16), pltpu.VMEM((2, 2, hb, hidden), BF16), pltpu.VMEM((2, 2, hb, hidden), BF16), pltpu.VMEM((2, hb, hidden), BF16), pltpu.VMEM((n_tok, hidden), BF16),
            pltpu.VMEM((2, hb, hidden), F32), pltpu.VMEM((2, hb, hidden), F32), pltpu.VMEM((n_tok, hidden), F32),
            dma((3,)),
        ] + [dma((8,))] * 6 + [dma((2, 2))] * 2 + [dma((2, 2, 2))] * 2 + [dma((3,))] * 2 + [dma((2, 2))] * 2,
        compiler_params=pltpu.CompilerParams(collective_id=0, has_side_effects=True, vmem_limit_bytes=46 << 20),
        name="moe",
    )(h2, ri, x1, *in_hbm([w_gate.reshape(e_local * hidden, ff), w_up.reshape(e_local * hidden, ff), w_down.reshape(e_local * ff, hidden)]))


def solution(mesh):
    ep_size = mesh.shape['ep']
    row_spec = P(('dp', 'ep'))
    replicated = P()
    expert_spec = P('ep')
    in_specs = (row_spec,) * 5 + (replicated,) * 9 + (expert_spec,) * 3

    def device_step(x_in, k_cache, v_cache, cache_len, topk_idx, ln_attn, w_q, w_k, w_v, q_norm, k_norm, w_o, ln_moe, w_router, w_gate, w_up, w_down):
        x1, h2, ri, k_new, v_new = attention(x_in, k_cache, v_cache, cache_len, topk_idx, ln_attn, w_q, w_k, w_v, q_norm, k_norm, w_o, ln_moe, w_router, ep_size)
        return moe(h2, ri, x1, w_gate, w_up, w_down, ep_size), k_new, v_new

    return jax.shard_map(device_step, mesh=mesh, in_specs=in_specs, out_specs=(row_spec,) * 3, check_vma=False)
```
